256 devices in a mesh: level: 2 (over x_hi), gx: 16 (over x_lo, z), gy: 8 (over y, core).
Axes of the slice: x: 4 (x_hi: 2, x_lo: 2; x = x_hi * 2 + x_lo), y: 4, z: 8, core: 2. Of those that a mesh axis runs over, the one named last changes fastest.
Arguments:
- u_init: float32 [128, 256, 256], P('gx', 'gy'), may hold values from -6 to 6
- v_init: float32 [128, 256, 256], P('gx', 'gy'), may hold values from -6 to 6
- speed_sq: float32 [128, 256, 256], P('gx', 'gy'), may hold values from 0.25 to 1
Outputs:
- final_u: float32 [2, 128, 256, 256], P('level', 'gx', 'gy')
- final_v: float32 [2, 128, 256, 256], P('level', 'gx', 'gy')
The draws below stay inside these ranges and needn't reach their ends.
All inputs are finite; a program needn't handle non-finite values.
Results may differ from the reference program's by a relative error of at most 0.00002.
Values sent between devices are 32-bit elements; how exact they have to be, the bound alone decides.
A program may use at most 64 MiB of HBM per device.

```python
import math
import jax
import jax.numpy as jnp

STEPS = 8
NX = 128
NY = 256
NZ = 256


def level_of(key, dims, cuts, least, top_value):
    def one(position, parts):
        heights = jax.random.uniform(jax.random.fold_in(jax.random.fold_in(key, 6), position), (parts,), jnp.float32, least / len(cuts), top_value / len(cuts))
        return jnp.repeat(jnp.exp(heights), dims[position] // parts).reshape((-1,) + (1,) * (len(dims) - position - 1))

    gain = one(*cuts[0])
    for cut in cuts[1:]:
        gain = gain * one(*cut)
    return gain


def normal_values(stream_key, extent, width, most, shards=(), kind=jnp.bfloat16):
    entries = width * jax.random.normal(stream_key, extent, jnp.float32)
    if shards:
        entries = entries * level_of(stream_key, extent, shards, -0.22, 0.18)
    return jnp.clip(entries, -most, most).astype(kind)


def setup_inputs(seed: int = 0) -> dict:
    splits = jax.random.split(jax.random.key(seed), 4)
    u_init = normal_values(splits[0], (NX, NY, NZ), 1.0, 6.0, ((0, 16), (1, 8)), jnp.float32)
    v_init = normal_values(splits[1], (NX, NY, NZ), 1.0, 6.0, ((0, 16), (1, 8)), jnp.float32)
    speed_sq = jnp.clip(jnp.exp(math.log(1.0) - 1.3862944 * jax.random.uniform(splits[2], (NX, NY, NZ), jnp.float32) ** level_of(splits[2], (NX, NY, NZ), ((0, 16), (1, 8)), -0.2, 0.2)), 0.25, 1.0)
    return {"u_init": u_init, "v_init": v_init, "speed_sq": speed_sq}


time_step = 0.12
half_step = 0.06
damping = 0.05


def laplace(field):
    total = -7.5 * field
    for axis in range(3):
        near = jnp.roll(field, 1, axis) + jnp.roll(field, -1, axis)
        far = jnp.roll(field, 2, axis) + jnp.roll(field, -2, axis)
        total = total + (4.0 / 3.0) * near - far / 12.0
    return total


def accel(disp, veloc, speed_sq):
    return speed_sq * laplace(disp) + damping * laplace(veloc)


def reference(u_init, v_init, speed_sq):
    pred_u, pred_v = u_init, v_init
    corr_u, corr_v = u_init, v_init
    accel_prev = accel(pred_u, pred_v, speed_sq)
    for moment in range(STEPS):
        next_u = pred_u + time_step * pred_v
        next_v = pred_v + time_step * accel_prev
        accel_next = accel(next_u, next_v, speed_sq)
        own_accel = accel(corr_u, corr_v, speed_sq)
        corr_u = corr_u + time_step * corr_v + half_step * (next_v - pred_v)
        corr_v = corr_v + time_step * own_accel + half_step * (accel_next - accel_prev)
        pred_u, pred_v, accel_prev = next_u, next_v, accel_next
    return jnp.stack([pred_u, corr_u]), jnp.stack([pred_v, corr_v])
```

```python
import functools

import jax
import jax.numpy as jnp
from jax import lax
from jax.experimental import pallas as pl
from jax.experimental.pallas import tpu as pltpu
from jax.sharding import PartitionSpec as P


H = 0.12
D = 0.05
W1 = 4.0 / 3.0
W2 = -1.0 / 12.0
ROUNDS = 3
MESH = pl.DeviceIdType.MESH
F32 = jnp.float32
XO, YO = 4, 8
OWN = slice(YO, YO + 32)
LO, HI = slice(0, 8), slice(40, 48)
DIAG = ((1, 1), (1, -1), (-1, 1), (-1, -1))


def rows(shape):
    return lax.broadcasted_iota(jnp.int32, shape, len(shape) - 2)


def turn(x, n):
    return pltpu.roll(x, n % 8, x.ndim - 2)


def from_below(c):
    r = rows(c.shape)
    return jnp.where(r == 0, W1 * turn(c, 1), 0.0) + jnp.where(r < 2, W2 * turn(c, 2), 0.0)


def from_above(c):
    r = rows(c.shape)
    return jnp.where(r == 7, W1 * turn(c, 7), 0.0) + jnp.where(r >= 6, W2 * turn(c, 6), 0.0)


def z_sums(a, b):
    lane = lax.broadcasted_iota(jnp.int32, a.shape, a.ndim - 1)
    ax = a.ndim - 1

    def shifted(n, mask):
        ra, rb = pltpu.roll(a, n % 128, ax), pltpu.roll(b, n % 128, ax)
        return jnp.where(mask, rb, ra), jnp.where(mask, ra, rb)

    l1, l2 = shifted(1, lane < 1), shifted(2, lane < 2)
    r1, r2 = shifted(127, lane >= 127), shifted(126, lane >= 126)
    return [(l1[i] + r1[i], l2[i] + r2[i]) for i in range(2)]


def lap(ref, p, lo, n, planes=None):
    at = (lambda q: q) if planes is None else (lambda q: pl.ds(q, planes))
    mid = [ref[at(p), f, lo : lo + n, :] for f in range(2)]
    zs = z_sums(*mid)
    out = []
    for f in range(2):
        near = zs[f][0] + ref[at(p - 1), f, lo : lo + n, :] + ref[at(p + 1), f, lo : lo + n, :]
        near = near + ref[at(p), f, lo - 1 : lo - 1 + n, :] + ref[at(p), f, lo + 1 : lo + 1 + n, :]
        far = zs[f][1] + ref[at(p - 2), f, lo : lo + n, :] + ref[at(p + 2), f, lo : lo + n, :]
        far = far + ref[at(p), f, lo - 2 : lo - 2 + n, :] + ref[at(p), f, lo + 2 : lo + 2 + n, :]
        out.append(W1 * near + (W2 * far - 7.5 * mid[f]))
    return out


def kernel(u_hbm, v_hbm, s_hbm, ou_hbm, ov_hbm, IU, I0, I1, I2, T0, T1, T2, TU, S, U, acc, A7, eW, eE, eS, eN, gW, gE, gS, gN,
           cs, cr, ob, lsem, ssem, rsem):
    level = lax.axis_index("level")
    gx, gy = lax.axis_index("gx"), lax.axis_index("gy")
    nx, ny = lax.axis_size("gx"), lax.axis_size("gy")

    def peer(dx, dy):
        return (level, lax.rem(gx + dx + nx, nx), lax.rem(gy + dy + ny, ny))

    around = ((1, 0), (-1, 0), (0, 1), (0, -1)) + DIAG
    barrier = pltpu.get_barrier_semaphore()
    for d in around:
        pl.semaphore_signal(barrier, 1, device_id=peer(*d), device_id_type=MESH)

    loads = []
    for src, dsts in ((v_hbm, ((I0, 2), (T0.at[0], XO))), (u_hbm, ((IU, 2), (TU, XO))), (s_hbm, ((S, XO),))):
        for dst, off in dsts:
            for f in range(2):
                copy = pltpu.make_async_copy(
                    src.at[:, :, 128 * f : 128 * f + 128], dst.at[off : off + 8, f, OWN, :], lsem.at[len(loads)]
                )
                copy.start()
                loads.append(copy)

    zero = jnp.zeros((2, 2, 48, 128), F32)
    for ref in (IU, I0, I1, I2):
        ref[0:2] = zero
        ref[10:12] = zero
        for sl in (LO, HI):
            ref[2:10, :, sl, :] = jnp.zeros((8, 2, 8, 128), F32)
    for ref in (eW, eE):
        ref[...] = jnp.zeros((6, 2, 48, 128), F32)
    for ref in (eS, eN):
        ref[...] = jnp.zeros((12, 2, 24, 128), F32)

    for copy in loads:
        copy.wait()
    pl.semaphore_wait(barrier, len(around))

    def send(r, slot, src, dst, dx, dy):
        copy = pltpu.make_async_remote_copy(
            src_ref=src, dst_ref=dst, send_sem=ssem.at[r, slot], recv_sem=rsem.at[r, slot],
            device_id=peer(dx, dy), device_id_type=MESH,
        )
        copy.start()
        return copy

    def send_x(r, slot, src, off, dst):
        return [
            send(r, slot, src.at[off + 6 : off + 8, :, OWN, :], dst.at[XO - 2 : XO, :, OWN, :], 1, 0),
            send(r, slot + 1, src.at[off : off + 2, :, OWN, :], dst.at[XO + 8 : XO + 10, :, OWN, :], -1, 0),
        ]

    def send_y(r, slot, src, off, dst):
        return [
            send(r, slot, src.at[off : off + 8, :, 32:40, :], dst.at[XO : XO + 8, :, LO, :], 0, 1),
            send(r, slot + 1, src.at[off : off + 8, :, 8:16, :], dst.at[XO : XO + 8, :, HI, :], 0, -1),
        ]

    def pack4(a, b, sy):
        r = rows(a.shape)
        return jnp.where(r >= 4 if sy > 0 else r < 4, b, turn(a, 4))

    def pack2(items, sy):
        r = rows(items[0].shape)
        out = items[0]
        for i in range(1, 4):
            first = ((6 if sy > 0 else 0) + 2 * i) % 8
            out = jnp.where((r == first) | (r == first + 1), turn(items[i], 2 * i), out)
        return out

    def corner(sx, sy):
        near = (6, 7) if sx > 0 else (0, 1)
        far = (4, 5) if sx > 0 else (2, 3)
        return near, far, (slice(32, 40) if sy > 0 else slice(8, 16))

    def corner_in(sx, sy):
        near = (XO - 2, XO - 1) if sx > 0 else (XO + 8, XO + 9)
        far = (XO - 4, XO - 3) if sx > 0 else (XO + 10, XO + 11)
        return near, far, (LO if sy > 0 else HI)

    waiting = []
    for r in range(ROUNDS):
        first, last = r == 0, r == ROUNDS - 1
        t0, t1, t2 = T0.at[r], T1.at[r], T2.at[r]
        sent = []
        x0 = send_x(r, 0, I0, 2, t0)
        y0 = send_y(r, 2, I0, 2, t0)
        extra = []
        if first:
            extra = send_x(r, 16, IU, 2, TU) + send_y(r, 18, IU, 2, TU)
            extra += send_x(r, 20, S, XO, S) + send_y(r, 22, S, XO, S)
            for i, sl in enumerate((slice(8, 16), slice(32, 40))):
                extra.append(send(r, 24 + 2 * i, S.at[XO + 4 : XO + 6, :, sl, :], S.at[XO - 4 : XO - 2, :, sl, :], 1, 0))
                extra.append(send(r, 25 + 2 * i, S.at[XO + 2 : XO + 4, :, sl, :], S.at[XO + 10 : XO + 12, :, sl, :], -1, 0))

            def start(p, c):
                for f, value in enumerate(lap(IU, p + 2, YO, 32)):
                    U[p, f] = value
                    acc[p, f] = IU[p + 2, f, OWN, :]
                return c

            lax.fori_loop(0, 8, start, 0)

        def alone1(p, c):
            for f, value in enumerate(lap(I0, p + 2, YO, 32)):
                I1[p + 2, f, OWN, :] = I0[p + 2, f, OWN, :] + H * (S[p + XO, f, OWN, :] * U[p, f] + D * value)
                U[p, f] = U[p, f] + H * value
            return c

        lax.fori_loop(0, 8, alone1, 0)
        x1 = send_x(r, 4, I1, 2, t1)
        y1 = send_y(r, 6, I1, 2, t1)
        diag = []
        for i, (sx, sy) in enumerate(DIAG):
            near, far, sl = corner(sx, sy)
            cs[i, 0] = pack4(*[I0[q + 2, :, sl, :] for q in near], sy)
            cs[i, 1] = pack2([I0[q + 2, :, sl, :] for q in far] + [I1[q + 2, :, sl, :] for q in near], sy)
            if first:
                cs[i, 2] = pack4(*[IU[q + 2, :, sl, :] for q in near], sy)
                cs[i, 3] = pack2([IU[q + 2, :, sl, :] for q in far] + [S[q + XO, :, sl, :] for q in near], sy)
            n = 4 if first else 2
            diag.append(send(r, 12 + i, cs.at[i, 0:n], cr.at[r, i, 0:n], sx, sy))

        def alone2(p, c):
            for f, value in enumerate(lap(I1, p + 2, YO, 32)):
                I2[p + 2, f, OWN, :] = I1[p + 2, f, OWN, :] + H * (S[p + XO, f, OWN, :] * U[p, f] + D * value)
            return c

        lax.fori_loop(0, 8, alone2, 0)
        x2 = send_x(r, 8, I2, 2, t2)
        y2 = send_y(r, 10, I2, 2, t2)

        for copy in y0 + x0 + extra:
            copy.wait()

        def own1(p, c):
            for f in range(2):
                for sl, cross, g in ((slice(8, 16), from_below, LO), (slice(32, 40), from_above, HI)):
                    k = slice(sl.start - YO, sl.stop - YO)
                    xv = cross(t0[p + XO, f, g, :])
                    add, grow = H * D * xv, H * xv
                    if first:
                        xu = cross(TU[p + XO, f, g, :])
                        add, grow = add + H * (S[p + XO, f, sl, :] * xu), grow + xu
                    t1[p + XO, f, sl, :] = I1[p + 2, f, sl, :] + add
                    U[p, f, k, :] = U[p, f, k, :] + grow
                t1[p + XO, f, 16:32, :] = I1[p + 2, f, 16:32, :]
            return c

        lax.fori_loop(0, 8, own1, 0)

        def cross_x(ref, x, sl):
            if x in (0, 8):
                a, b = (-1, -2) if x == 0 else (7, 6)
            elif x in (-1, 7):
                a, b = (0, 1) if x == -1 else (8, 9)
            else:
                return W2 * ref[{1: -1, -2: 0, 6: 8, 9: 7}[x] + XO, :, sl, :]
            return W1 * ref[a + XO, :, sl, :] + W2 * ref[b + XO, :, sl, :]

        for x in (0, 1, 6, 7):
            xv = cross_x(t0, x, OWN)
            add, grow = H * D * xv, H * xv
            if first:
                xu = cross_x(TU, x, OWN)
                add, grow = add + H * (S[x + XO, :, OWN, :] * xu), grow + xu
            t1[x + XO, :, OWN, :] = t1[x + XO, :, OWN, :] + add
            U[x] = U[x] + grow

        for copy in diag:
            copy.wait()
        for i, (sx, sy) in enumerate(DIAG):
            near, far, sl = corner_in(sx, sy)
            for k, ref in ((0, t0), (2, TU))[: 2 if first else 1]:
                ref[near[1], :, sl, :] = cr[r, i, k]
                ref[near[0], :, sl, :] = turn(cr[r, i, k], 4)
                ref[far[0], :, sl, :] = cr[r, i, k + 1]
                ref[far[1], :, sl, :] = turn(cr[r, i, k + 1], 6)
            for k, ref in ((1, t1), (3, S))[: 2 if first else 1]:
                ref[near[0], :, sl, :] = turn(cr[r, i, k], 4)
                ref[near[1], :, sl, :] = turn(cr[r, i, k], 2)

        def both(cross, *where):
            xv = cross(t0)
            e, g = H * D * xv, H * xv
            if first:
                xu = cross(TU)
                e, g = e + H * (S[where] * xu), g + xu
            return e, g

        every = slice(None)
        for side, (e_ref, g_ref, near, far) in enumerate(
            ((eW, gW, (-2, -1), (-4, -3)), (eE, gE, (8, 9), (10, 11)))
        ):
            base = -4 if side == 0 else 6
            for x in near:
                e, g = both(lambda ref: cross_x(ref, x, OWN), x + XO, every, OWN)
                e_ref[x - base, :, OWN, :] = e
                g_ref[x - near[0]] = g
            for x in near + far:
                for sl, cross, g_sl in ((slice(8, 16), from_below, LO), (slice(32, 40), from_above, HI)):
                    e, g = both(lambda ref: cross(ref[x + XO, :, g_sl, :]), x + XO, every, sl)
                    if x in near:
                        k = slice(sl.start - YO, sl.stop - YO)
                        e_ref[x - base, :, sl, :] = e_ref[x - base, :, sl, :] + e
                        g_ref[x - near[0], :, k, :] = g_ref[x - near[0], :, k, :] + g
                    else:
                        e_ref[x - base, :, sl, :] = e
        sides = ((eS, gS, LO, from_above, slice(8, 16)), (eN, gN, HI, from_below, slice(32, 40)))
        mid = slice(XO, XO + 8)
        for e_ref, g_ref, sl, cross, o_sl in sides:
            e, g = both(lambda ref: cross(ref[mid, :, o_sl, :]), mid, every, sl)
            e_ref[2:10, :, 8:16, :] = e
            g_ref[...] = g
            for x in (0, 1, 6, 7):
                e, g = both(lambda ref: cross_x(ref, x, sl), x + XO, every, sl)
                e_ref[x + 2, :, 8:16, :] = e_ref[x + 2, :, 8:16, :] + e
                g_ref[x] = g_ref[x] + g
            for x in (-2, -1, 8, 9):
                e, g = both(lambda ref: cross_x(ref, x, sl) + cross(ref[x + XO, :, o_sl, :]), x + XO, every, sl)
                t1[x + XO, :, sl, :] = t1[x + XO, :, sl, :] + e

        for copy in y1 + x1:
            copy.wait()
        for e_ref, x, k in ((eW, XO - 2, 2), (eE, XO + 8, 2)):
            t1[x : x + 2, :, OWN, :] = t1[x : x + 2, :, OWN, :] + e_ref[k : k + 2, :, OWN, :]
        for e_ref, g_ref, sl, cross, o_sl in sides:
            t1[mid, :, sl, :] = t1[mid, :, sl, :] + e_ref[2:10, :, 8:16, :]

        def own2(p, c):
            for f, value in enumerate(lap(t1, p + XO, YO, 32)):
                s, u = S[p + XO, f, OWN, :], U[p, f]
                a = s * u + D * value
                t2[p + XO, f, OWN, :] = t1[p + XO, f, OWN, :] + H * a
                if last:
                    A7[p, f] = a
                U[p, f] = u + H * value
            return c

        lax.fori_loop(0, 8, own2, 0)

        for e_ref, g_ref, near, base in ((eW, gW, (-2, -1), -4), (eE, gE, (8, 9), 6)):
            for x in near:
                value = lap(e_ref, x - base, YO, 32) if True else None
                cx = cross_x(t1, x, OWN)
                for f in range(2):
                    full = value[f] + cx[f]
                    low = full[0:8] + from_below(t1[x + XO, f, LO, :])
                    high = full[24:32] + from_above(t1[x + XO, f, HI, :])
                    full = jnp.concatenate([low, full[8:24], high], axis=0)
                    e = e_ref[x - base, f, OWN, :] + H * (S[x + XO, f, OWN, :] * g_ref[x - near[0], f] + D * full)
                    g_ref[x - near[0], f] = e
        for e_ref, g_ref, sl, cross, o_sl in sides:
            value = lap(e_ref, 2, 8, 8, planes=8)
            for f in range(2):
                full = value[f] + cross(t1[mid, f, o_sl, :])
                e = e_ref[2:10, f, 8:16, :] + H * (S[mid, f, sl, :] * g_ref[:, f] + D * full)
                g_ref[:, f] = e
            for x in (0, 1, 6, 7):
                g_ref[x] = g_ref[x] + H * D * cross_x(t1, x, sl)

        for copy in y2 + x2:
            copy.wait()
        for g_ref, x in ((gW, XO - 2), (gE, XO + 8)):
            t2[x : x + 2, :, OWN, :] = t2[x : x + 2, :, OWN, :] + g_ref[...]
        for e_ref, g_ref, sl, cross, o_sl in sides:
            t2[mid, :, sl, :] = t2[mid, :, sl, :] + g_ref[...]

        if not last:
            nxt = T0.at[r + 1]

            def own3(p, c):
                for f, value in enumerate(lap(t2, p + XO, YO, 32)):
                    u, mine = U[p, f], t2[p + XO, f, OWN, :]
                    new = mine + H * (S[p + XO, f, OWN, :] * u + D * value)
                    I0[p + 2, f, OWN, :] = new
                    nxt[p + XO, f, OWN, :] = new
                    U[p, f] = u + H * value
                    acc[p, f] = acc[p, f] + H * (t0[p + XO, f, OWN, :] + t1[p + XO, f, OWN, :] + mine)
                return c

            lax.fori_loop(0, 8, own3, 0)
        else:
            raised = level == 1

            def finish(p, c):
                for f, value in enumerate(lap(t2, p + XO, YO, 32)):
                    v7, v8 = t1[p + XO, f, OWN, :], t2[p + XO, f, OWN, :]
                    a8 = S[p + XO, f, OWN, :] * U[p, f] + D * value
                    u8 = acc[p, f] + H * (t0[p + XO, f, OWN, :] + v7)
                    ob[0, p, f] = jnp.where(raised, u8 + 4 * H * (v8 - v7), u8)
                    ob[1, p, f] = jnp.where(raised, v8 + 4 * H * (a8 - A7[p, f]), v8)
                return c

            lax.fori_loop(0, 8, finish, 0)
    stores = []
    for i, dst in enumerate((ou_hbm, ov_hbm)):
        for f in range(2):
            copy = pltpu.make_async_copy(ob.at[i, :, f], dst.at[0, :, :, 128 * f : 128 * f + 128], lsem.at[2 * i + f])
            copy.start()
            stores.append(copy)
    for copy in stores:
        copy.wait()


def body(u, v, s):
    ext, alone, block = (16, 2, 48, 128), (12, 2, 48, 128), (8, 2, 32, 128)
    vm = lambda *shape: pltpu.VMEM(shape, F32)
    scratch = [vm(*alone)] * 4 + [vm(ROUNDS, *ext)] * 3 + [vm(*ext)] * 2 + [vm(*block)] * 3
    scratch += [vm(6, 2, 48, 128)] * 2 + [vm(12, 2, 24, 128)] * 2
    scratch += [vm(2, 2, 32, 128)] * 2 + [vm(8, 2, 8, 128)] * 2
    scratch += [vm(4, 4, 2, 8, 128), vm(ROUNDS, 4, 4, 2, 8, 128), vm(2, *block)]
    scratch += [pltpu.SemaphoreType.DMA((10,)), pltpu.SemaphoreType.DMA((ROUNDS, 28)), pltpu.SemaphoreType.DMA((ROUNDS, 28))]
    out = jax.ShapeDtypeStruct((1, 8, 32, 256), F32)
    return pl.pallas_call(
        kernel,
        out_shape=(out, out),
        in_specs=[pl.BlockSpec(memory_space=pl.ANY)] * 3,
        out_specs=(pl.BlockSpec(memory_space=pl.ANY),) * 2,
        scratch_shapes=scratch,
        compiler_params=pltpu.CompilerParams(collective_id=0, has_side_effects=True, vmem_limit_bytes=48 * 1024 * 1024),
    )(u, v, s)


def solution(mesh):
    placed = (P("gx", "gy", None),) * 3
    return jax.shard_map(
        body,
        mesh=mesh,
        in_specs=placed,
        out_specs=(P("level", "gx", "gy", None),) * 2,
        check_vma=False,
    )
```

```python
import functools

import jax
import jax.numpy as jnp
from jax import lax
from jax.experimental import pallas as pl
from jax.experimental.pallas import tpu as pltpu
from jax.sharding import PartitionSpec as P


H = 0.12
D = 0.05
W1 = 4.0 / 3.0
W2 = -1.0 / 12.0
ROUNDS = 3
MESH = pl.DeviceIdType.MESH
F32 = jnp.float32
XO, YO = 4, 8
OWN = slice(YO, YO + 32)
LO, HI = slice(0, 8), slice(40, 48)
RING = (-2, -1, 8, 9)
NEAREST = {0: (-1, -2), -1: (0, 1), 7: (8, 9), 8: (7, 6)}
NEXT = {1: -1, -2: 0, 6: 8, 9: 7}
DIAG = ((1, 1), (1, -1), (-1, 1), (-1, -1))


def rows(shape):
    return lax.broadcasted_iota(jnp.int32, shape, len(shape) - 2)


def turn(x, n):
    return pltpu.roll(x, n % 8, x.ndim - 2)


def from_below(c):
    r = rows(c.shape)
    return jnp.where(r == 0, W1 * turn(c, 1), 0.0) + jnp.where(r < 2, W2 * turn(c, 2), 0.0)


def from_above(c):
    r = rows(c.shape)
    return jnp.where(r == 7, W1 * turn(c, 7), 0.0) + jnp.where(r >= 6, W2 * turn(c, 6), 0.0)


def z_sums(a, b):
    lane = lax.broadcasted_iota(jnp.int32, a.shape, a.ndim - 1)
    ax = a.ndim - 1

    def shifted(n, mask):
        ra, rb = pltpu.roll(a, n % 128, ax), pltpu.roll(b, n % 128, ax)
        return jnp.where(mask, rb, ra), jnp.where(mask, ra, rb)

    l1, l2 = shifted(1, lane < 1), shifted(2, lane < 2)
    r1, r2 = shifted(127, lane >= 127), shifted(126, lane >= 126)
    return [(l1[i] + r1[i], l2[i] + r2[i]) for i in range(2)]


def lap(ref, p, lo, n, planes=None):
    at = (lambda q: q) if planes is None else (lambda q: pl.ds(q, planes))
    mid = [ref[at(p), f, lo : lo + n, :] for f in range(2)]
    zs = z_sums(*mid)
    out = []
    for f in range(2):
        near = zs[f][0] + ref[at(p - 1), f, lo : lo + n, :] + ref[at(p + 1), f, lo : lo + n, :]
        near = near + ref[at(p), f, lo - 1 : lo - 1 + n, :] + ref[at(p), f, lo + 1 : lo + 1 + n, :]
        far = zs[f][1] + ref[at(p - 2), f, lo : lo + n, :] + ref[at(p + 2), f, lo : lo + n, :]
        far = far + ref[at(p), f, lo - 2 : lo - 2 + n, :] + ref[at(p), f, lo + 2 : lo + 2 + n, :]
        out.append(W1 * near + (W2 * far - 7.5 * mid[f]))
    return out


def kernel(u_hbm, v_hbm, s_hbm, out_u, out_v, IU, I0, I1, I2, J1, J2, T0, T1, T2, TU, S, U, acc, A7, eW, eE, eS, eN, gW, gE,
           gS, gN, cs, cr, lsem, ssem, rsem):
    level = lax.axis_index("level")
    gx, gy = lax.axis_index("gx"), lax.axis_index("gy")
    nx, ny = lax.axis_size("gx"), lax.axis_size("gy")

    def peer(dx, dy):
        return (level, lax.rem(gx + dx + nx, nx), lax.rem(gy + dy + ny, ny))

    around = ((1, 0), (-1, 0), (0, 1), (0, -1)) + DIAG
    barrier = pltpu.get_barrier_semaphore()
    for d in around:
        pl.semaphore_signal(barrier, 1, device_id=peer(*d), device_id_type=MESH)

    loads = []
    for src, dst, off in ((v_hbm, I0, 2), (u_hbm, IU, 2), (s_hbm, S, XO)):
        for f in range(2):
            copy = pltpu.make_async_copy(
                src.at[:, :, 128 * f : 128 * f + 128], dst.at[off : off + 8, f, OWN, :], lsem.at[len(loads)]
            )
            copy.start()
            loads.append(copy)

    zero = jnp.zeros((2, 2, 48, 128), F32)
    for ref in (IU, I0, I1, I2, J1, J2):
        ref[0:2] = zero
        ref[10:12] = zero
        for sl in (LO, HI):
            ref[2:10, :, sl, :] = jnp.zeros((8, 2, 8, 128), F32)
    for ref in (eW, eE):
        ref[...] = jnp.zeros((6, 2, 48, 128), F32)
    for ref in (eS, eN):
        ref[...] = jnp.zeros((12, 2, 24, 128), F32)

    for copy in loads:
        copy.wait()

    def send(r, slot, src, dst, dx, dy):
        got = slot + 16 * (r % 2) if slot < 16 else slot + 16
        copy = pltpu.make_async_remote_copy(
            src_ref=src, dst_ref=dst, send_sem=ssem.at[slot], recv_sem=rsem.at[got],
            device_id=peer(dx, dy), device_id_type=MESH,
        )
        copy.start()
        return copy

    def send_x(r, slot, src, off, dst):
        return [
            send(r, slot, src.at[off + 6 : off + 8, :, OWN, :], dst.at[XO - 2 : XO, :, OWN, :], 1, 0),
            send(r, slot + 1, src.at[off : off + 2, :, OWN, :], dst.at[XO + 8 : XO + 10, :, OWN, :], -1, 0),
        ]

    def send_y(r, slot, src, off, dst):
        return [
            send(r, slot, src.at[off : off + 8, :, 32:40, :], dst.at[XO : XO + 8, :, LO, :], 0, 1),
            send(r, slot + 1, src.at[off : off + 8, :, 8:16, :], dst.at[XO : XO + 8, :, HI, :], 0, -1),
        ]

    def pack4(a, b, sy):
        r = rows(a.shape)
        return jnp.where(r >= 4 if sy > 0 else r < 4, b, turn(a, 4))

    def pack2(items, sy):
        r = rows(items[0].shape)
        out = items[0]
        for i in range(1, 4):
            first = ((6 if sy > 0 else 0) + 2 * i) % 8
            out = jnp.where((r == first) | (r == first + 1), turn(items[i], 2 * i), out)
        return out

    def corner(sx, sy):
        near = (6, 7) if sx > 0 else (0, 1)
        far = (4, 5) if sx > 0 else (2, 3)
        return near, far, (slice(32, 40) if sy > 0 else slice(8, 16))

    def corner_in(sx, sy):
        near = (XO - 2, XO - 1) if sx > 0 else (XO + 8, XO + 9)
        far = (XO - 4, XO - 3) if sx > 0 else (XO + 10, XO + 11)
        return near, far, (LO if sy > 0 else HI)

    def start(p, c):
        for f, value in enumerate(lap(IU, p + 2, YO, 32)):
            U[p, f] = value
            acc[p, f] = IU[p + 2, f, OWN, :]
        return c

    def alone1(p, c):
        for f, value in enumerate(lap(I0, p + 2, YO, 32)):
            u = U[p, f]
            new = I0[p + 2, f, OWN, :] + H * (S[p + XO, f, OWN, :] * u + D * value)
            I1[p + 2, f, OWN, :] = new
            J1[p + 2, f, OWN, :] = new
            U[p, f] = u + H * value
        return c

    def alone2(p, c):
        for f, value in enumerate(lap(I1, p + 2, YO, 32)):
            I2[p + 2, f, OWN, :] = I1[p + 2, f, OWN, :] + H * (S[p + XO, f, OWN, :] * U[p, f] + D * value)
        return c

    def cross_x(own, ring, x, sl):
        at = (lambda q: own[q + 2, :, OWN, :]) if sl is OWN and x in RING else (lambda q: ring[q + XO, :, sl, :])
        if x in NEAREST:
            a, b = NEAREST[x]
            return W1 * at(a) + W2 * at(b)
        return W2 * at(NEXT[x])

    ends = ((slice(8, 16), from_below, LO), (slice(32, 40), from_above, HI))

    def fix_ends(ring, p, put):
        for sl, cross, g in ends:
            put(p, sl, lambda ref: cross(ref[p + XO, :, g, :]))

    def fix_faces(ring, put):
        for x in (0, 1, 6, 7):
            put(x, OWN, lambda ref: cross_x(None, ref, x, OWN))
            fix_ends(ring, x, put)

    def fix_inner(ring, put):
        def step(p, c):
            fix_ends(ring, p, put)
            return c

        lax.fori_loop(2, 6, step, 0)

    def off(sl):
        return slice(sl.start - YO, sl.stop - YO)

    def pack(i, first):
        sx, sy = DIAG[i]
        near, far, sl = corner(sx, sy)
        cs[i, 0] = pack4(*[I0[q + 2, :, sl, :] for q in near], sy)
        cs[i, 1] = pack2([I0[q + 2, :, sl, :] for q in far] + [I1[q + 2, :, sl, :] for q in near], sy)
        if first:
            cs[i, 2] = pack4(*[IU[q + 2, :, sl, :] for q in near], sy)
            cs[i, 3] = pack2([IU[q + 2, :, sl, :] for q in far] + [S[q + XO, :, sl, :] for q in near], sy)

    def send_diag(r, n):
        return [send(r, 12 + i, cs.at[i, 0:n], cr.at[r, i, 0:n], *DIAG[i]) for i in range(4)]

    def faces_first(step):
        lax.fori_loop(0, 4, lambda i, c: step(i + 4 * (i // 2), c), 0)

    def inner(step):
        lax.fori_loop(2, 6, step, 0)

    x0 = y0 = None
    for r in range(ROUNDS):
        first, last = r == 0, r == ROUNDS - 1
        t0, t1, t2 = T0.at[r], T1.at[r], T2.at[r]
        extra = []
        if first:
            pl.semaphore_wait(barrier, len(around))
            x0 = send_x(r, 0, I0, 2, t0)
            y0 = send_y(r, 2, I0, 2, t0)
            extra = send_x(r, 16, IU, 2, TU) + send_y(r, 18, IU, 2, TU)
            extra += send_x(r, 20, S, XO, S) + send_y(r, 22, S, XO, S)
            for i, sl in enumerate((slice(8, 16), slice(32, 40))):
                extra.append(send(r, 24 + 2 * i, S.at[XO + 4 : XO + 6, :, sl, :], S.at[XO - 4 : XO - 2, :, sl, :], 1, 0))
                extra.append(send(r, 25 + 2 * i, S.at[XO + 2 : XO + 4, :, sl, :], S.at[XO + 10 : XO + 12, :, sl, :], -1, 0))
            lax.fori_loop(0, 8, start, 0)
        faces_first(alone1)
        x1 = send_x(r, 4, I1, 2, t1)
        for i in range(4):
            pack(i, first)
        diag = send_diag(r, 4 if first else 2)
        inner(alone1)
        y1 = send_y(r, 6, I1, 2, t1)
        faces_first(alone2)
        x2 = send_x(r, 8, I2, 2, t2)
        inner(alone2)
        y2 = send_y(r, 10, I2, 2, t2)

        for copy in y0 + x0 + extra:
            copy.wait()

        def put1(p, sl, cross):
            xv = cross(t0)
            add, grow = H * D * xv, H * xv
            if first:
                xu = cross(TU)
                add, grow = add + H * (S[p + XO, :, sl, :] * xu), grow + xu
            J1[p + 2, :, sl, :] = J1[p + 2, :, sl, :] + add
            U[p, :, off(sl), :] = U[p, :, off(sl), :] + grow

        fix_faces(t0, put1)
        fix_inner(t0, put1)

        def own2(p, c):
            for f, value in enumerate(lap(J1, p + 2, YO, 32)):
                u = U[p, f]
                a = S[p + XO, f, OWN, :] * u + D * value
                J2[p + 2, f, OWN, :] = J1[p + 2, f, OWN, :] + H * a
                if last:
                    A7[p, f] = a
                U[p, f] = u + H * value
            return c

        lax.fori_loop(0, 8, own2, 0)

        for copy in diag:
            copy.wait()
        for i, (sx, sy) in enumerate(DIAG):
            near, far, sl = corner_in(sx, sy)
            for k, ref in ((0, t0), (2, TU))[: 2 if first else 1]:
                ref[near[1], :, sl, :] = cr[r, i, k]
                ref[near[0], :, sl, :] = turn(cr[r, i, k], 4)
                ref[far[0], :, sl, :] = cr[r, i, k + 1]
                ref[far[1], :, sl, :] = turn(cr[r, i, k + 1], 6)
            for k, ref in ((1, t1), (3, S))[: 2 if first else 1]:
                ref[near[0], :, sl, :] = turn(cr[r, i, k], 4)
                ref[near[1], :, sl, :] = turn(cr[r, i, k], 2)

        def both(cross, *where):
            xv = cross(I0, t0)
            e, g = H * D * xv, H * xv
            if first:
                xu = cross(IU, TU)
                e, g = e + H * (S[where] * xu), g + xu
            return e, g

        every = slice(None)
        for e_ref, g_ref, near, far, base in ((eW, gW, (-2, -1), (-4, -3), -4), (eE, gE, (8, 9), (10, 11), 6)):
            for x in near:
                e, g = both(lambda own, ring: cross_x(own, ring, x, OWN), x + XO, every, OWN)
                e_ref[x - base, :, OWN, :] = e
                g_ref[x - near[0]] = g
            for x in near + far:
                for sl, cross, g_sl in ends:
                    e, g = both(lambda own, ring: cross(ring[x + XO, :, g_sl, :]), x + XO, every, sl)
                    if x in near:
                        e_ref[x - base, :, sl, :] = e_ref[x - base, :, sl, :] + e
                        g_ref[x - near[0], :, off(sl), :] = g_ref[x - near[0], :, off(sl), :] + g
                    else:
                        e_ref[x - base, :, sl, :] = e
        sides = ((eS, gS, LO, from_above, slice(8, 16)), (eN, gN, HI, from_below, slice(32, 40)))
        mid = slice(XO, XO + 8)
        for e_ref, g_ref, sl, cross, o_sl in sides:
            e, g = both(lambda own, ring: cross(own[2:10, :, o_sl, :]), mid, every, sl)
            e_ref[2:10, :, 8:16, :] = e
            g_ref[...] = g
            for x in (0, 1, 6, 7):
                e, g = both(lambda own, ring: cross_x(own, ring, x, sl), x + XO, every, sl)
                e_ref[x + 2, :, 8:16, :] = e_ref[x + 2, :, 8:16, :] + e
                g_ref[x] = g_ref[x] + g
            for x in RING:
                e, g = both(
                    lambda own, ring: cross_x(own, ring, x, sl) + cross(ring[x + XO, :, o_sl, :]), x + XO, every, sl
                )
                t1[x + XO, :, sl, :] = t1[x + XO, :, sl, :] + e

        for e_ref, g_ref, near, base in ((eW, gW, (-2, -1), -4), (eE, gE, (8, 9), 6)):
            for x in near:
                value = lap(e_ref, x - base, YO, 32)
                cx = cross_x(J1, t1, x, OWN)
                for f in range(2):
                    full = value[f] + cx[f]
                    low = full[0:8] + from_below(t1[x + XO, f, LO, :])
                    high = full[24:32] + from_above(t1[x + XO, f, HI, :])
                    full = jnp.concatenate([low, full[8:24], high], axis=0)
                    e = e_ref[x - base, f, OWN, :] + H * (S[x + XO, f, OWN, :] * g_ref[x - near[0], f] + D * full)
                    g_ref[x - near[0], f] = e
        for e_ref, g_ref, sl, cross, o_sl in sides:
            value = lap(e_ref, 2, 8, 8, planes=8)
            for f in range(2):
                full = value[f] + cross(J1[2:10, f, o_sl, :])
                e = e_ref[2:10, f, 8:16, :] + H * (S[mid, f, sl, :] * g_ref[:, f] + D * full)
                g_ref[:, f] = e
            for x in (0, 1, 6, 7):
                g_ref[x] = g_ref[x] + H * D * cross_x(None, t1, x, sl)

        for copy in y1 + x1:
            copy.wait()
        for e_ref, x, k in ((eW, XO - 2, 2), (eE, XO + 8, 2)):
            t1[x : x + 2, :, OWN, :] = t1[x : x + 2, :, OWN, :] + e_ref[k : k + 2, :, OWN, :]
        for e_ref, g_ref, sl, cross, o_sl in sides:
            t1[mid, :, sl, :] = t1[mid, :, sl, :] + e_ref[2:10, :, 8:16, :]

        def put2(p, sl, cross):
            xv = cross(t1)
            J2[p + 2, :, sl, :] = J2[p + 2, :, sl, :] + H * D * xv
            U[p, :, off(sl), :] = U[p, :, off(sl), :] + H * xv
            if last:
                A7[p, :, off(sl), :] = A7[p, :, off(sl), :] + D * xv

        fix_faces(t1, put2)
        fix_inner(t1, put2)

        raised = level == 1

        def own3(p, c):
            for f, value in enumerate(lap(J2, p + 2, YO, 32)):
                u, v8, v7 = U[p, f], J2[p + 2, f, OWN, :], J1[p + 2, f, OWN, :]
                a8 = S[p + XO, f, OWN, :] * u + D * value
                if last:
                    u8 = acc[p, f] + H * (I0[p + 2, f, OWN, :] + v7)
                    lanes = slice(128 * f, 128 * f + 128)
                    out_u[0, p, :, lanes] = jnp.where(raised, u8 + 4 * H * (v8 - v7), u8)
                    out_v[0, p, :, lanes] = jnp.where(raised, v8 + 4 * H * (a8 - A7[p, f]), v8)
                else:
                    acc[p, f] = acc[p, f] + H * (I0[p + 2, f, OWN, :] + v7 + v8)
                    I0[p + 2, f, OWN, :] = v8 + H * a8
                    U[p, f] = u + H * value
            return c

        lax.fori_loop(0, 8, own3, 0)

        for copy in y2 + x2:
            copy.wait()
        for g_ref, x in ((gW, XO - 2), (gE, XO + 8)):
            t2[x : x + 2, :, OWN, :] = t2[x : x + 2, :, OWN, :] + g_ref[...]
        for e_ref, g_ref, sl, cross, o_sl in sides:
            t2[mid, :, sl, :] = t2[mid, :, sl, :] + g_ref[...]

        def put3(p, sl, cross):
            xv = cross(t2)
            if last:
                for f in range(2):
                    lanes = slice(128 * f, 128 * f + 128)
                    old = out_v[0, p, off(sl), lanes]
                    out_v[0, p, off(sl), lanes] = jnp.where(raised, old + 4 * H * D * xv[f], old)
            else:
                I0[p + 2, :, sl, :] = I0[p + 2, :, sl, :] + H * D * xv
                U[p, :, off(sl), :] = U[p, :, off(sl), :] + H * xv

        fix_faces(t2, put3)
        if not last:
            x0 = send_x(r + 1, 0, I0, 2, T0.at[r + 1])
        fix_inner(t2, put3)
        if not last:
            y0 = send_y(r + 1, 2, I0, 2, T0.at[r + 1])


def body(u, v, s):
    ext, alone, block = (16, 2, 48, 128), (12, 2, 48, 128), (8, 2, 32, 128)
    vm = lambda *shape: pltpu.VMEM(shape, F32)
    scratch = [vm(*alone)] * 6 + [vm(ROUNDS, *ext)] * 3 + [vm(*ext)] * 2 + [vm(*block)] * 3
    scratch += [vm(6, 2, 48, 128)] * 2 + [vm(12, 2, 24, 128)] * 2
    scratch += [vm(2, 2, 32, 128)] * 2 + [vm(8, 2, 8, 128)] * 2
    scratch += [vm(4, 4, 2, 8, 128), vm(ROUNDS, 4, 4, 2, 8, 128)]
    scratch += [pltpu.SemaphoreType.DMA((6,)), pltpu.SemaphoreType.DMA((28,)), pltpu.SemaphoreType.DMA((44,))]
    out = jax.ShapeDtypeStruct((1, 8, 32, 256), F32)
    return pl.pallas_call(
        kernel,
        out_shape=(out, out),
        in_specs=[pl.BlockSpec(memory_space=pltpu.HBM)] * 3,
        out_specs=(pl.BlockSpec(memory_space=pltpu.VMEM),) * 2,
        scratch_shapes=scratch,
        compiler_params=pltpu.CompilerParams(collective_id=0, has_side_effects=True, vmem_limit_bytes=48 * 1024 * 1024),
    )(*[pltpu.with_memory_space_constraint(x, pltpu.HBM) for x in (u, v, s)])


def solution(mesh):
    placed = (P("gx", "gy", None),) * 3
    return jax.shard_map(
        body,
        mesh=mesh,
        in_specs=placed,
        out_specs=(P("level", "gx", "gy", None),) * 2,
        check_vma=False,
    )
```

```python
import functools

import jax
import jax.numpy as jnp
from jax import lax
from jax.experimental import pallas as pl
from jax.experimental.pallas import tpu as pltpu
from jax.sharding import PartitionSpec as P


H = 0.12
D = 0.05
W1 = 4.0 / 3.0
W2 = -1.0 / 12.0
ROUNDS = 3
MESH = pl.DeviceIdType.MESH
F32 = jnp.float32
XO, YO = 4, 8
OWN = slice(YO, YO + 32)
LO, HI = slice(0, 8), slice(40, 48)
RING = (-2, -1, 8, 9)
NEAREST = {0: (-1, -2), -1: (0, 1), 7: (8, 9), 8: (7, 6)}
NEXT = {1: -1, -2: 0, 6: 8, 9: 7}
DIAG = ((1, 1), (1, -1), (-1, 1), (-1, -1))


def rows(shape):
    return lax.broadcasted_iota(jnp.int32, shape, len(shape) - 2)


def turn(x, n):
    return pltpu.roll(x, n % 8, x.ndim - 2)


def from_below(c):
    r = rows(c.shape)
    return jnp.where(r == 0, W1 * turn(c, 1), 0.0) + jnp.where(r < 2, W2 * turn(c, 2), 0.0)


def from_above(c):
    r = rows(c.shape)
    return jnp.where(r == 7, W1 * turn(c, 7), 0.0) + jnp.where(r >= 6, W2 * turn(c, 6), 0.0)


def z_sums(a, b):
    lane = lax.broadcasted_iota(jnp.int32, a.shape, a.ndim - 1)
    ax = a.ndim - 1

    def shifted(n, mask):
        ra, rb = pltpu.roll(a, n % 128, ax), pltpu.roll(b, n % 128, ax)
        return jnp.where(mask, rb, ra), jnp.where(mask, ra, rb)

    l1, l2 = shifted(1, lane < 1), shifted(2, lane < 2)
    r1, r2 = shifted(127, lane >= 127), shifted(126, lane >= 126)
    return [(l1[i] + r1[i], l2[i] + r2[i]) for i in range(2)]


def lap(ref, p, lo, n, planes=None):
    at = (lambda q: q) if planes is None else (lambda q: pl.ds(q, planes))
    mid = [ref[at(p), f, lo : lo + n, :] for f in range(2)]
    zs = z_sums(*mid)
    out = []
    for f in range(2):
        near = zs[f][0] + ref[at(p - 1), f, lo : lo + n, :] + ref[at(p + 1), f, lo : lo + n, :]
        near = near + ref[at(p), f, lo - 1 : lo - 1 + n, :] + ref[at(p), f, lo + 1 : lo + 1 + n, :]
        far = zs[f][1] + ref[at(p - 2), f, lo : lo + n, :] + ref[at(p + 2), f, lo : lo + n, :]
        far = far + ref[at(p), f, lo - 2 : lo - 2 + n, :] + ref[at(p), f, lo + 2 : lo + 2 + n, :]
        out.append(W1 * near + (W2 * far - 7.5 * mid[f]))
    return out


def kernel(u_hbm, v_hbm, s_hbm, out_u, out_v, IU, I0, I1, I2, J1, J2, T0, T1, T2, TU, S, U, acc, A7, eW, eE, eS, eN, gW, gE,
           gS, gN, cs, cr, fs, fr, lsem, ssem, rsem):
    level = lax.axis_index("level")
    gx, gy = lax.axis_index("gx"), lax.axis_index("gy")
    nx, ny = lax.axis_size("gx"), lax.axis_size("gy")

    def peer(dx, dy):
        return (level, lax.rem(gx + dx + nx, nx), lax.rem(gy + dy + ny, ny))

    around = ((1, 0), (-1, 0), (0, 1), (0, -1)) + DIAG
    barrier = pltpu.get_barrier_semaphore()
    for d in around:
        pl.semaphore_signal(barrier, 1, device_id=peer(*d), device_id_type=MESH)

    loads = []
    for src, dst, off in ((v_hbm, I0, 2), (u_hbm, IU, 2), (s_hbm, S, XO)):
        for f in range(2):
            copy = pltpu.make_async_copy(
                src.at[:, :, 128 * f : 128 * f + 128], dst.at[off : off + 8, f, OWN, :], lsem.at[len(loads)]
            )
            copy.start()
            loads.append(copy)

    zero = jnp.zeros((2, 2, 48, 128), F32)
    for ref in (IU, I0, I1, I2, J1, J2):
        ref[0:2] = zero
        ref[10:12] = zero
        for sl in (LO, HI):
            ref[2:10, :, sl, :] = jnp.zeros((8, 2, 8, 128), F32)
    for ref in (eW, eE):
        ref[...] = jnp.zeros((6, 2, 48, 128), F32)
    for ref in (eS, eN):
        ref[...] = jnp.zeros((12, 2, 24, 128), F32)

    for copy in loads:
        copy.wait()

    def send(r, slot, src, dst, dx, dy):
        got = slot + 20 * (r % 2) if slot < 20 else slot + 20
        copy = pltpu.make_async_remote_copy(
            src_ref=src, dst_ref=dst, send_sem=ssem.at[slot], recv_sem=rsem.at[got],
            device_id=peer(dx, dy), device_id_type=MESH,
        )
        copy.start()
        return copy

    def send_x(r, slot, src, off, dst):
        return [
            send(r, slot, src.at[off + 6 : off + 8, :, OWN, :], dst.at[XO - 2 : XO, :, OWN, :], 1, 0),
            send(r, slot + 1, src.at[off : off + 2, :, OWN, :], dst.at[XO + 8 : XO + 10, :, OWN, :], -1, 0),
        ]

    def send_y(r, slot, src, off, dst):
        return [
            send(r, slot, src.at[off : off + 8, :, 32:40, :], dst.at[XO : XO + 8, :, LO, :], 0, 1),
            send(r, slot + 1, src.at[off : off + 8, :, 8:16, :], dst.at[XO : XO + 8, :, HI, :], 0, -1),
        ]

    def pack4(a, b, sy):
        r = rows(a.shape)
        return jnp.where(r >= 4 if sy > 0 else r < 4, b, turn(a, 4))

    def pack2(items, sy):
        r = rows(items[0].shape)
        out = items[0]
        for i in range(1, 4):
            first = ((6 if sy > 0 else 0) + 2 * i) % 8
            out = jnp.where((r == first) | (r == first + 1), turn(items[i], 2 * i), out)
        return out

    def corner(sx, sy):
        near = (6, 7) if sx > 0 else (0, 1)
        far = (4, 5) if sx > 0 else (2, 3)
        return near, far, (slice(32, 40) if sy > 0 else slice(8, 16))

    def corner_in(sx, sy):
        near = (XO - 2, XO - 1) if sx > 0 else (XO + 8, XO + 9)
        far = (XO - 4, XO - 3) if sx > 0 else (XO + 10, XO + 11)
        return near, far, (LO if sy > 0 else HI)

    def start(p, c):
        for f, value in enumerate(lap(IU, p + 2, YO, 32)):
            U[p, f] = value
            acc[p, f] = IU[p + 2, f, OWN, :]
        return c

    def alone1(p, c):
        for f, value in enumerate(lap(I0, p + 2, YO, 32)):
            u = U[p, f]
            new = I0[p + 2, f, OWN, :] + H * (S[p + XO, f, OWN, :] * u + D * value)
            I1[p + 2, f, OWN, :] = new
            J1[p + 2, f, OWN, :] = new
            U[p, f] = u + H * value
        return c

    def alone2(p, c):
        for f, value in enumerate(lap(I1, p + 2, YO, 32)):
            I2[p + 2, f, OWN, :] = I1[p + 2, f, OWN, :] + H * (S[p + XO, f, OWN, :] * U[p, f] + D * value)
        return c

    def cross_x(own, ring, x, sl):
        at = (lambda q: own[q + 2, :, OWN, :]) if sl is OWN and x in RING else (lambda q: ring[q + XO, :, sl, :])
        if x in NEAREST:
            a, b = NEAREST[x]
            return W1 * at(a) + W2 * at(b)
        return W2 * at(NEXT[x])

    ends = ((slice(8, 16), from_below, LO), (slice(32, 40), from_above, HI))

    def fix_ends(ring, p, put):
        for sl, cross, g in ends:
            put(p, sl, lambda ref: cross(ref[p + XO, :, g, :]))

    def fix_faces(ring, put):
        for x in (0, 1, 6, 7):
            put(x, OWN, lambda ref: cross_x(None, ref, x, OWN))
            fix_ends(ring, x, put)

    def fix_inner(ring, put):
        def step(p, c):
            fix_ends(ring, p, put)
            return c

        lax.fori_loop(2, 6, step, 0)

    def off(sl):
        return slice(sl.start - YO, sl.stop - YO)

    def halves(ref, planes, shift, sl):
        return [ref[q + shift, f, sl, :] for f in range(2) for q in planes]

    def pack(i, first):
        sx, sy = DIAG[i]
        near, far, sl = corner(sx, sy)
        for k, ref in ((0, I0), (3, IU))[: 2 if first else 1]:
            for f in range(2):
                cs[i, k + f] = pack4(*[ref[q + 2, f, sl, :] for q in near], sy)
            cs[i, k + 2] = pack2(halves(ref, far, 2, sl), sy)
        if first:
            cs[i, 6] = pack2(halves(S, near, XO, sl), sy)

    def send_corners(r, n):
        return [send(r, 12 + i, cs.at[i, 0:n], cr.at[r, i, 0:n], *DIAG[i]) for i in range(4)]

    def send_corners1(r):
        copies = []
        for i, (sx, sy) in enumerate(DIAG):
            near, far, sl = corner(sx, sy)
            cs[i, 7] = pack2(halves(I1, near, 2, sl), sy)
            copies.append(send(r, 16 + i, cs.at[i, 7:8], cr.at[r, i, 7:8], sx, sy))
        return copies

    def unpack2(tile):
        return [[turn(tile, -2 * (q + 2 * f)) for f in range(2)] for q in range(2)]

    def faces_first(step):
        lax.fori_loop(0, 4, lambda i, c: step(i + 4 * (i // 2), c), 0)

    def inner(step):
        lax.fori_loop(2, 6, step, 0)

    x0 = y0 = None
    for r in range(ROUNDS):
        first, last = r == 0, r == ROUNDS - 1
        t0, t1, t2 = T0.at[r], T1.at[r], T2.at[r]
        extra = []
        if first:
            for k, planes in enumerate(((4, 5), (2, 3))):
                for f in range(2):
                    a, b, c, d = [S[q + XO, f, sl, :] for q in planes for sl in (slice(8, 16), slice(32, 40))]
                    i = rows(a.shape)
                    fs[k, f] = jnp.where(i < 2, a, jnp.where(i >= 6, b, jnp.where(i < 4, turn(c, 2), turn(d, 6))))
            for i in range(4):
                pack(i, True)
            pl.semaphore_wait(barrier, len(around))
            x0 = send_x(r, 0, I0, 2, t0)
            y0 = send_y(r, 2, I0, 2, t0)
            extra = send_x(r, 20, IU, 2, TU) + send_y(r, 22, IU, 2, TU)
            diag = send_corners(r, 7)
            extra += send_x(r, 24, S, XO, S) + send_y(r, 26, S, XO, S)
            extra += [send(r, 28, fs.at[0], fr.at[0], 1, 0), send(r, 29, fs.at[1], fr.at[1], -1, 0)]
            lax.fori_loop(0, 8, start, 0)
        faces_first(alone1)
        x1 = send_x(r, 4, I1, 2, t1)
        diag1 = send_corners1(r)
        inner(alone1)
        y1 = send_y(r, 6, I1, 2, t1)
        faces_first(alone2)
        x2 = send_x(r, 8, I2, 2, t2)
        inner(alone2)
        y2 = send_y(r, 10, I2, 2, t2)

        for copy in y0 + x0 + extra:
            copy.wait()

        def put1(p, sl, cross):
            xv = cross(t0)
            add, grow = H * D * xv, H * xv
            if first:
                xu = cross(TU)
                add, grow = add + H * (S[p + XO, :, sl, :] * xu), grow + xu
            J1[p + 2, :, sl, :] = J1[p + 2, :, sl, :] + add
            U[p, :, off(sl), :] = U[p, :, off(sl), :] + grow

        fix_faces(t0, put1)
        fix_inner(t0, put1)

        def own2(p, c):
            for f, value in enumerate(lap(J1, p + 2, YO, 32)):
                u = U[p, f]
                a = S[p + XO, f, OWN, :] * u + D * value
                J2[p + 2, f, OWN, :] = J1[p + 2, f, OWN, :] + H * a
                if last:
                    A7[p, f] = a
                U[p, f] = u + H * value
            return c

        lax.fori_loop(0, 8, own2, 0)

        for copy in diag:
            copy.wait()
        for i, (sx, sy) in enumerate(DIAG):
            near, far, sl = corner_in(sx, sy)
            for k, ref in ((0, t0), (3, TU))[: 2 if first else 1]:
                ends2 = unpack2(cr[r, i, k + 2])
                for f in range(2):
                    ref[near[1], f, sl, :] = cr[r, i, k + f]
                    ref[near[0], f, sl, :] = turn(cr[r, i, k + f], 4)
                    ref[far[0], f, sl, :] = ends2[0][f]
                    ref[far[1], f, sl, :] = ends2[1][f]
            if first:
                ends2 = unpack2(cr[r, i, 6])
                for q in range(2):
                    for f in range(2):
                        S[near[q], f, sl, :] = ends2[q][f]
        if first:
            for k, x in enumerate((XO - 4, XO + 10)):
                for f in range(2):
                    S[x, f, 8:16, :] = fr[k, f]
                    S[x, f, 32:40, :] = fr[k, f]
                    S[x + 1, f, 8:16, :] = turn(fr[k, f], 6)
                    S[x + 1, f, 32:40, :] = turn(fr[k, f], 2)

        def both(cross, *where):
            xv = cross(I0, t0)
            e, g = H * D * xv, H * xv
            if first:
                xu = cross(IU, TU)
                e, g = e + H * (S[where] * xu), g + xu
            return e, g

        every = slice(None)
        for e_ref, g_ref, near, far, base in ((eW, gW, (-2, -1), (-4, -3), -4), (eE, gE, (8, 9), (10, 11), 6)):
            for x in near:
                e, g = both(lambda own, ring: cross_x(own, ring, x, OWN), x + XO, every, OWN)
                e_ref[x - base, :, OWN, :] = e
                g_ref[x - near[0]] = g
            for x in near + far:
                for sl, cross, g_sl in ends:
                    e, g = both(lambda own, ring: cross(ring[x + XO, :, g_sl, :]), x + XO, every, sl)
                    if x in near:
                        e_ref[x - base, :, sl, :] = e_ref[x - base, :, sl, :] + e
                        g_ref[x - near[0], :, off(sl), :] = g_ref[x - near[0], :, off(sl), :] + g
                    else:
                        e_ref[x - base, :, sl, :] = e
        sides = ((eS, gS, LO, from_above, slice(8, 16)), (eN, gN, HI, from_below, slice(32, 40)))
        mid = slice(XO, XO + 8)
        for e_ref, g_ref, sl, cross, o_sl in sides:
            e, g = both(lambda own, ring: cross(own[2:10, :, o_sl, :]), mid, every, sl)
            e_ref[2:10, :, 8:16, :] = e
            g_ref[...] = g
            for x in (0, 1, 6, 7):
                e, g = both(lambda own, ring: cross_x(own, ring, x, sl), x + XO, every, sl)
                e_ref[x + 2, :, 8:16, :] = e_ref[x + 2, :, 8:16, :] + e
                g_ref[x] = g_ref[x] + g
            for x in RING:
                e, g = both(
                    lambda own, ring: cross_x(own, ring, x, sl) + cross(ring[x + XO, :, o_sl, :]), x + XO, every, sl
                )
                t1[x + XO, :, sl, :] = e

        for e_ref, g_ref, near, base in ((eW, gW, (-2, -1), -4), (eE, gE, (8, 9), 6)):
            for x in near:
                value = lap(e_ref, x - base, YO, 32)
                cx = cross_x(J1, t1, x, OWN)
                for f in range(2):
                    full = value[f] + cx[f]
                    e = e_ref[x - base, f, OWN, :] + H * (S[x + XO, f, OWN, :] * g_ref[x - near[0], f] + D * full)
                    g_ref[x - near[0], f] = e
        for e_ref, g_ref, sl, cross, o_sl in sides:
            value = lap(e_ref, 2, 8, 8, planes=8)
            for f in range(2):
                full = value[f] + cross(J1[2:10, f, o_sl, :])
                e = e_ref[2:10, f, 8:16, :] + H * (S[mid, f, sl, :] * g_ref[:, f] + D * full)
                g_ref[:, f] = e

        for copy in y1 + x1:
            copy.wait()
        for e_ref, x, k in ((eW, XO - 2, 2), (eE, XO + 8, 2)):
            t1[x : x + 2, :, OWN, :] = t1[x : x + 2, :, OWN, :] + e_ref[k : k + 2, :, OWN, :]
        for e_ref, g_ref, sl, cross, o_sl in sides:
            t1[mid, :, sl, :] = t1[mid, :, sl, :] + e_ref[2:10, :, 8:16, :]

        def put2(p, sl, cross):
            xv = cross(t1)
            J2[p + 2, :, sl, :] = J2[p + 2, :, sl, :] + H * D * xv
            U[p, :, off(sl), :] = U[p, :, off(sl), :] + H * xv
            if last:
                A7[p, :, off(sl), :] = A7[p, :, off(sl), :] + D * xv

        fix_faces(t1, put2)
        fix_inner(t1, put2)

        raised = level == 1

        def own3(p, c):
            for f, value in enumerate(lap(J2, p + 2, YO, 32)):
                u, v8, v7 = U[p, f], J2[p + 2, f, OWN, :], J1[p + 2, f, OWN, :]
                a8 = S[p + XO, f, OWN, :] * u + D * value
                if last:
                    u8 = acc[p, f] + H * (I0[p + 2, f, OWN, :] + v7)
                    lanes = slice(128 * f, 128 * f + 128)
                    out_u[0, p, :, lanes] = jnp.where(raised, u8 + 4 * H * (v8 - v7), u8)
                    out_v[0, p, :, lanes] = jnp.where(raised, v8 + 4 * H * (a8 - A7[p, f]), v8)
                else:
                    acc[p, f] = acc[p, f] + H * (I0[p + 2, f, OWN, :] + v7 + v8)
                    I0[p + 2, f, OWN, :] = v8 + H * a8
                    U[p, f] = u + H * value
            return c

        lax.fori_loop(0, 8, own3, 0)

        for copy in diag1:
            copy.wait()
        for i, (sx, sy) in enumerate(DIAG):
            near, far, sl = corner_in(sx, sy)
            ends2 = unpack2(cr[r, i, 7])
            for q in range(2):
                for f in range(2):
                    t1[near[q], f, sl, :] = t1[near[q], f, sl, :] + ends2[q][f]
        for g_ref, near in ((gW, (-2, -1)), (gE, (8, 9))):
            for x in near:
                for sl, cross, g_sl in ends:
                    q = x - near[0]
                    g_ref[q, :, off(sl), :] = g_ref[q, :, off(sl), :] + H * D * cross(t1[x + XO, :, g_sl, :])
        for e_ref, g_ref, sl, cross, o_sl in sides:
            for x in (0, 1, 6, 7):
                g_ref[x] = g_ref[x] + H * D * cross_x(None, t1, x, sl)

        for copy in y2 + x2:
            copy.wait()
        for g_ref, x in ((gW, XO - 2), (gE, XO + 8)):
            t2[x : x + 2, :, OWN, :] = t2[x : x + 2, :, OWN, :] + g_ref[...]
        for e_ref, g_ref, sl, cross, o_sl in sides:
            t2[mid, :, sl, :] = t2[mid, :, sl, :] + g_ref[...]

        def put3(p, sl, cross):
            xv = cross(t2)
            if last:
                for f in range(2):
                    lanes = slice(128 * f, 128 * f + 128)
                    old = out_v[0, p, off(sl), lanes]
                    out_v[0, p, off(sl), lanes] = jnp.where(raised, old + 4 * H * D * xv[f], old)
            else:
                I0[p + 2, :, sl, :] = I0[p + 2, :, sl, :] + H * D * xv
                U[p, :, off(sl), :] = U[p, :, off(sl), :] + H * xv

        fix_faces(t2, put3)
        if not last:
            x0 = send_x(r + 1, 0, I0, 2, T0.at[r + 1])
        fix_inner(t2, put3)
        if not last:
            for i in range(4):
                pack(i, False)
            diag = send_corners(r + 1, 3)
            y0 = send_y(r + 1, 2, I0, 2, T0.at[r + 1])


def body(u, v, s):
    ext, alone, block = (16, 2, 48, 128), (12, 2, 48, 128), (8, 2, 32, 128)
    vm = lambda *shape: pltpu.VMEM(shape, F32)
    scratch = [vm(*alone)] * 6 + [vm(ROUNDS, *ext)] * 3 + [vm(*ext)] * 2 + [vm(*block)] * 3
    scratch += [vm(6, 2, 48, 128)] * 2 + [vm(12, 2, 24, 128)] * 2
    scratch += [vm(2, 2, 32, 128)] * 2 + [vm(8, 2, 8, 128)] * 2
    scratch += [vm(4, 8, 8, 128), vm(ROUNDS, 4, 8, 8, 128), vm(2, 2, 8, 128), vm(2, 2, 8, 128)]
    scratch += [pltpu.SemaphoreType.DMA((6,)), pltpu.SemaphoreType.DMA((30,)), pltpu.SemaphoreType.DMA((50,))]
    out = jax.ShapeDtypeStruct((1, 8, 32, 256), F32)
    return pl.pallas_call(
        kernel,
        out_shape=(out, out),
        in_specs=[pl.BlockSpec(memory_space=pltpu.HBM)] * 3,
        out_specs=(pl.BlockSpec(memory_space=pltpu.VMEM),) * 2,
        scratch_shapes=scratch,
        compiler_params=pltpu.CompilerParams(collective_id=0, has_side_effects=True, vmem_limit_bytes=48 * 1024 * 1024),
    )(*[pltpu.with_memory_space_constraint(x, pltpu.HBM) for x in (u, v, s)])


def solution(mesh):
    placed = (P("gx", "gy", None),) * 3
    return jax.shard_map(
        body,
        mesh=mesh,
        in_specs=placed,
        out_specs=(P("level", "gx", "gy", None),) * 2,
        check_vma=False,
    )
```

```python
import functools

import jax
import jax.numpy as jnp
from jax import lax
from jax.experimental import pallas as pl
from jax.experimental.pallas import tpu as pltpu
from jax.sharding import PartitionSpec as P


H = 0.12
D = 0.05
W1 = 4.0 / 3.0
W2 = -1.0 / 12.0
ROUNDS = 3
MESH = pl.DeviceIdType.MESH
F32 = jnp.float32
XO, YO = 4, 8
OWN = slice(YO, YO + 32)
LO, HI = slice(0, 8), slice(40, 48)
RING = (-2, -1, 8, 9)
NEAREST = {0: (-1, -2), -1: (0, 1), 7: (8, 9), 8: (7, 6)}
NEXT = {1: -1, -2: 0, 6: 8, 9: 7}
DIAG = ((1, 1), (1, -1), (-1, 1), (-1, -1))


def rows(shape):
    return lax.broadcasted_iota(jnp.int32, shape, len(shape) - 2)


def turn(x, n):
    return pltpu.roll(x, n % 8, x.ndim - 2)


def from_below(c):
    r = rows(c.shape)
    return jnp.where(r == 0, W1 * turn(c, 1), 0.0) + jnp.where(r < 2, W2 * turn(c, 2), 0.0)


def from_above(c):
    r = rows(c.shape)
    return jnp.where(r == 7, W1 * turn(c, 7), 0.0) + jnp.where(r >= 6, W2 * turn(c, 6), 0.0)


def z_sums(a, b):
    lane = lax.broadcasted_iota(jnp.int32, a.shape, a.ndim - 1)
    ax = a.ndim - 1

    def shifted(n, mask):
        ra, rb = pltpu.roll(a, n % 128, ax), pltpu.roll(b, n % 128, ax)
        return jnp.where(mask, rb, ra), jnp.where(mask, ra, rb)

    l1, l2 = shifted(1, lane < 1), shifted(2, lane < 2)
    r1, r2 = shifted(127, lane >= 127), shifted(126, lane >= 126)
    return [(l1[i] + r1[i], l2[i] + r2[i]) for i in range(2)]


def lap(ref, p, lo, n, planes=None):
    at = (lambda q: q) if planes is None else (lambda q: pl.ds(q, planes))
    mid = [ref[at(p), f, lo : lo + n, :] for f in range(2)]
    zs = z_sums(*mid)
    out = []
    for f in range(2):
        near = zs[f][0] + ref[at(p - 1), f, lo : lo + n, :] + ref[at(p + 1), f, lo : lo + n, :]
        near = near + ref[at(p), f, lo - 1 : lo - 1 + n, :] + ref[at(p), f, lo + 1 : lo + 1 + n, :]
        far = zs[f][1] + ref[at(p - 2), f, lo : lo + n, :] + ref[at(p + 2), f, lo : lo + n, :]
        far = far + ref[at(p), f, lo - 2 : lo - 2 + n, :] + ref[at(p), f, lo + 2 : lo + 2 + n, :]
        out.append(W1 * near + (W2 * far - 7.5 * mid[f]))
    return out


def lap_z(ref, p, zs):
    out = []
    for f in range(2):
        mid = ref[p, f, OWN, :]
        near = ref[p - 1, f, OWN, :] + ref[p + 1, f, OWN, :]
        near = near + (ref[p, f, YO - 1 : YO + 31, :] + ref[p, f, YO + 1 : YO + 33, :])
        far = ref[p - 2, f, OWN, :] + ref[p + 2, f, OWN, :]
        far = far + (ref[p, f, YO - 2 : YO + 30, :] + ref[p, f, YO + 2 : YO + 34, :])
        out.append(W1 * near + (W2 * far - 5.0 * mid) + (1.0 / 12.0) * zs[f])
    return out


def kernel(u_hbm, v_hbm, s_hbm, out_u, out_v, IU, I0, I1, I2, J1, J2, T0, T1, T2, TU, S, U, acc, A7, eW, eE, eS, eN, gW, gE,
           gS, gN, cs, cr, fs, fr, Z, band, lsem, ssem, rsem):
    level = lax.axis_index("level")
    gx, gy = lax.axis_index("gx"), lax.axis_index("gy")
    nx, ny = lax.axis_size("gx"), lax.axis_size("gy")

    def peer(dx, dy):
        return (level, lax.rem(gx + dx + nx, nx), lax.rem(gy + dy + ny, ny))

    around = ((1, 0), (-1, 0), (0, 1), (0, -1)) + DIAG
    barrier = pltpu.get_barrier_semaphore()
    for d in around:
        pl.semaphore_signal(barrier, 1, device_id=peer(*d), device_id_type=MESH)

    loads = []
    for src, dst, off in ((v_hbm, I0, 2), (u_hbm, IU, 2), (s_hbm, S, XO)):
        for f in range(2):
            copy = pltpu.make_async_copy(
                src.at[:, :, 128 * f : 128 * f + 128], dst.at[off : off + 8, f, OWN, :], lsem.at[len(loads)]
            )
            copy.start()
            loads.append(copy)

    zero = jnp.zeros((2, 2, 48, 128), F32)
    for ref in (IU, I0, I1, I2, J1, J2):
        ref[0:2] = zero
        ref[10:12] = zero
        for sl in (LO, HI):
            ref[2:10, :, sl, :] = jnp.zeros((8, 2, 8, 128), F32)
    for ref in (eW, eE):
        ref[...] = jnp.zeros((6, 2, 48, 128), F32)
    for ref in (eS, eN):
        ref[...] = jnp.zeros((12, 2, 24, 128), F32)

    gap = lax.broadcasted_iota(jnp.int32, (256, 256), 0) - lax.broadcasted_iota(jnp.int32, (256, 256), 1)
    gap = jnp.abs(gap)
    gap = jnp.minimum(gap, 256 - gap)
    weight = jnp.where(gap == 0, -30.0, jnp.where(gap == 1, 16.0, jnp.where(gap == 2, -1.0, 0.0)))
    band[...] = weight.astype(jnp.bfloat16)

    for copy in loads:
        copy.wait()

    def along_z(ref, planes):
        rest = jnp.concatenate(
            [jnp.concatenate([ref[p + 2, f, OWN, :] for f in range(2)], axis=1) for p in planes], axis=0
        )
        parts = []
        for _ in range(3):
            parts.append(rest.astype(jnp.bfloat16))
            rest = rest - parts[-1].astype(F32)
        n = 32 * len(planes)
        out = jnp.dot(jnp.concatenate(parts, axis=0), band[...], preferred_element_type=F32)
        out = out[0:n] + (out[n : 2 * n] + out[2 * n : 3 * n])
        for i, p in enumerate(planes):
            for f in range(2):
                Z[p, f] = out[32 * i : 32 * i + 32, 128 * f : 128 * f + 128]

    def send(r, slot, src, dst, dx, dy):
        got = slot + 20 * (r % 2) if slot < 20 else slot + 20
        copy = pltpu.make_async_remote_copy(
            src_ref=src, dst_ref=dst, send_sem=ssem.at[slot], recv_sem=rsem.at[got],
            device_id=peer(dx, dy), device_id_type=MESH,
        )
        copy.start()
        return copy

    def send_x(r, slot, src, off, dst):
        return [
            send(r, slot, src.at[off + 6 : off + 8, :, OWN, :], dst.at[XO - 2 : XO, :, OWN, :], 1, 0),
            send(r, slot + 1, src.at[off : off + 2, :, OWN, :], dst.at[XO + 8 : XO + 10, :, OWN, :], -1, 0),
        ]

    def send_y(r, slot, src, off, dst):
        return [
            send(r, slot, src.at[off : off + 8, :, 32:40, :], dst.at[XO : XO + 8, :, LO, :], 0, 1),
            send(r, slot + 1, src.at[off : off + 8, :, 8:16, :], dst.at[XO : XO + 8, :, HI, :], 0, -1),
        ]

    def pack4(a, b, sy):
        r = rows(a.shape)
        return jnp.where(r >= 4 if sy > 0 else r < 4, b, turn(a, 4))

    def pack2(items, sy):
        r = rows(items[0].shape)
        out = items[0]
        for i in range(1, 4):
            first = ((6 if sy > 0 else 0) + 2 * i) % 8
            out = jnp.where((r == first) | (r == first + 1), turn(items[i], 2 * i), out)
        return out

    def corner(sx, sy):
        near = (6, 7) if sx > 0 else (0, 1)
        far = (4, 5) if sx > 0 else (2, 3)
        return near, far, (slice(32, 40) if sy > 0 else slice(8, 16))

    def corner_in(sx, sy):
        near = (XO - 2, XO - 1) if sx > 0 else (XO + 8, XO + 9)
        far = (XO - 4, XO - 3) if sx > 0 else (XO + 10, XO + 11)
        return near, far, (LO if sy > 0 else HI)

    def start(p, c):
        for f, value in enumerate(lap_z(IU, p + 2, Z[p])):
            U[p, f] = value
            acc[p, f] = IU[p + 2, f, OWN, :]
        return c

    def alone1(p, c):
        for f, value in enumerate(lap_z(I0, p + 2, Z[p])):
            u = U[p, f]
            new = I0[p + 2, f, OWN, :] + H * (S[p + XO, f, OWN, :] * u + D * value)
            I1[p + 2, f, OWN, :] = new
            J1[p + 2, f, OWN, :] = new
            U[p, f] = u + H * value
        return c

    def alone2(p, c):
        for f, value in enumerate(lap_z(I1, p + 2, Z[p])):
            I2[p + 2, f, OWN, :] = I1[p + 2, f, OWN, :] + H * (S[p + XO, f, OWN, :] * U[p, f] + D * value)
        return c

    def cross_x(own, ring, x, sl):
        at = (lambda q: own[q + 2, :, OWN, :]) if sl is OWN and x in RING else (lambda q: ring[q + XO, :, sl, :])
        if x in NEAREST:
            a, b = NEAREST[x]
            return W1 * at(a) + W2 * at(b)
        return W2 * at(NEXT[x])

    ends = ((slice(8, 16), from_below, LO), (slice(32, 40), from_above, HI))

    def fix_ends(ring, p, put):
        for sl, cross, g in ends:
            put(p, sl, lambda ref: cross(ref[p + XO, :, g, :]))

    def fix_faces(ring, put):
        for x in (0, 1, 6, 7):
            put(x, OWN, lambda ref: cross_x(None, ref, x, OWN))
            fix_ends(ring, x, put)

    def fix_inner(ring, put):
        def step(p, c):
            fix_ends(ring, p, put)
            return c

        lax.fori_loop(2, 6, step, 0, unroll=4)

    def off(sl):
        return slice(sl.start - YO, sl.stop - YO)

    def halves(ref, planes, shift, sl):
        return [ref[q + shift, f, sl, :] for f in range(2) for q in planes]

    def pack(i, first):
        sx, sy = DIAG[i]
        near, far, sl = corner(sx, sy)
        for k, ref in ((0, I0), (3, IU))[: 2 if first else 1]:
            for f in range(2):
                cs[i, k + f] = pack4(*[ref[q + 2, f, sl, :] for q in near], sy)
            cs[i, k + 2] = pack2(halves(ref, far, 2, sl), sy)
        if first:
            cs[i, 6] = pack2(halves(S, near, XO, sl), sy)

    def send_corners(r, n):
        return [send(r, 12 + i, cs.at[i, 0:n], cr.at[r, i, 0:n], *DIAG[i]) for i in range(4)]

    def send_corners1(r):
        copies = []
        for i, (sx, sy) in enumerate(DIAG):
            near, far, sl = corner(sx, sy)
            cs[i, 7] = pack2(halves(I1, near, 2, sl), sy)
            copies.append(send(r, 16 + i, cs.at[i, 7:8], cr.at[r, i, 7:8], sx, sy))
        return copies

    def unpack2(tile):
        return [[turn(tile, -2 * (q + 2 * f)) for f in range(2)] for q in range(2)]

    def faces_first(step, ref):
        along_z(ref, (0, 1, 6, 7))
        lax.fori_loop(0, 4, lambda i, c: step(i + 4 * (i // 2), c), 0, unroll=4)

    def inner(step, ref):
        along_z(ref, (2, 3, 4, 5))
        lax.fori_loop(2, 6, step, 0, unroll=4)

    x0 = y0 = None
    for r in range(ROUNDS):
        first, last = r == 0, r == ROUNDS - 1
        t0, t1, t2 = T0.at[r], T1.at[r], T2.at[r]
        extra = []
        if first:
            for k, planes in enumerate(((4, 5), (2, 3))):
                for f in range(2):
                    a, b, c, d = [S[q + XO, f, sl, :] for q in planes for sl in (slice(8, 16), slice(32, 40))]
                    i = rows(a.shape)
                    fs[k, f] = jnp.where(i < 2, a, jnp.where(i >= 6, b, jnp.where(i < 4, turn(c, 2), turn(d, 6))))
            for i in range(4):
                pack(i, True)
            pl.semaphore_wait(barrier, len(around))
            x0 = send_x(r, 0, I0, 2, t0)
            y0 = send_y(r, 2, I0, 2, t0)
            extra = send_x(r, 20, IU, 2, TU) + send_y(r, 22, IU, 2, TU)
            diag = send_corners(r, 7)
            extra += send_x(r, 24, S, XO, S) + send_y(r, 26, S, XO, S)
            extra += [send(r, 28, fs.at[0], fr.at[0], 1, 0), send(r, 29, fs.at[1], fr.at[1], -1, 0)]
            faces_first(start, IU)
            inner(start, IU)
        faces_first(alone1, I0)
        diag1 = send_corners1(r)
        x1 = send_x(r, 4, I1, 2, t1)
        inner(alone1, I0)
        y1 = send_y(r, 6, I1, 2, t1)
        faces_first(alone2, I1)
        x2 = send_x(r, 8, I2, 2, t2)
        inner(alone2, I1)
        y2 = send_y(r, 10, I2, 2, t2)

        for copy in y0 + x0 + extra:
            copy.wait()

        def put1(p, sl, cross):
            xv = cross(t0)
            add, grow = H * D * xv, H * xv
            if first:
                xu = cross(TU)
                add, grow = add + H * (S[p + XO, :, sl, :] * xu), grow + xu
            J1[p + 2, :, sl, :] = J1[p + 2, :, sl, :] + add
            U[p, :, off(sl), :] = U[p, :, off(sl), :] + grow

        fix_faces(t0, put1)
        fix_inner(t0, put1)

        def own2(p, c):
            for f, value in enumerate(lap_z(J1, p + 2, Z[p])):
                u = U[p, f]
                a = S[p + XO, f, OWN, :] * u + D * value
                J2[p + 2, f, OWN, :] = J1[p + 2, f, OWN, :] + H * a
                if last:
                    A7[p, f] = a
                U[p, f] = u + H * value
            return c

        faces_first(own2, J1)
        inner(own2, J1)

        for copy in diag:
            copy.wait()
        for i, (sx, sy) in enumerate(DIAG):
            near, far, sl = corner_in(sx, sy)
            for k, ref in ((0, t0), (3, TU))[: 2 if first else 1]:
                ends2 = unpack2(cr[r, i, k + 2])
                for f in range(2):
                    ref[near[1], f, sl, :] = cr[r, i, k + f]
                    ref[near[0], f, sl, :] = turn(cr[r, i, k + f], 4)
                    ref[far[0], f, sl, :] = ends2[0][f]
                    ref[far[1], f, sl, :] = ends2[1][f]
            if first:
                ends2 = unpack2(cr[r, i, 6])
                for q in range(2):
                    for f in range(2):
                        S[near[q], f, sl, :] = ends2[q][f]
        if first:
            for k, x in enumerate((XO - 4, XO + 10)):
                for f in range(2):
                    S[x, f, 8:16, :] = fr[k, f]
                    S[x, f, 32:40, :] = fr[k, f]
                    S[x + 1, f, 8:16, :] = turn(fr[k, f], 6)
                    S[x + 1, f, 32:40, :] = turn(fr[k, f], 2)

        def both(cross, *where):
            xv = cross(I0, t0)
            e, g = H * D * xv, H * xv
            if first:
                xu = cross(IU, TU)
                e, g = e + H * (S[where] * xu), g + xu
            return e, g

        every = slice(None)
        for e_ref, g_ref, near, far, base in ((eW, gW, (-2, -1), (-4, -3), -4), (eE, gE, (8, 9), (10, 11), 6)):
            for x in near:
                e, g = both(lambda own, ring: cross_x(own, ring, x, OWN), x + XO, every, OWN)
                e_ref[x - base, :, OWN, :] = e
                g_ref[x - near[0]] = g
            for x in near + far:
                for sl, cross, g_sl in ends:
                    e, g = both(lambda own, ring: cross(ring[x + XO, :, g_sl, :]), x + XO, every, sl)
                    if x in near:
                        e_ref[x - base, :, sl, :] = e_ref[x - base, :, sl, :] + e
                        g_ref[x - near[0], :, off(sl), :] = g_ref[x - near[0], :, off(sl), :] + g
                    else:
                        e_ref[x - base, :, sl, :] = e
        sides = ((eS, gS, LO, from_above, slice(8, 16)), (eN, gN, HI, from_below, slice(32, 40)))
        mid = slice(XO, XO + 8)
        for e_ref, g_ref, sl, cross, o_sl in sides:
            e, g = both(lambda own, ring: cross(own[2:10, :, o_sl, :]), mid, every, sl)
            e_ref[2:10, :, 8:16, :] = e
            g_ref[...] = g
            for x in (0, 1, 6, 7):
                e, g = both(lambda own, ring: cross_x(own, ring, x, sl), x + XO, every, sl)
                e_ref[x + 2, :, 8:16, :] = e_ref[x + 2, :, 8:16, :] + e
                g_ref[x] = g_ref[x] + g
            for x in RING:
                e, g = both(
                    lambda own, ring: cross_x(own, ring, x, sl) + cross(ring[x + XO, :, o_sl, :]), x + XO, every, sl
                )
                t1[x + XO, :, sl, :] = e

        for e_ref, g_ref, near, base in ((eW, gW, (-2, -1), -4), (eE, gE, (8, 9), 6)):
            for x in near:
                value = lap(e_ref, x - base, YO, 32)
                cx = cross_x(J1, t1, x, OWN)
                for f in range(2):
                    full = value[f] + cx[f]
                    e = e_ref[x - base, f, OWN, :] + H * (S[x + XO, f, OWN, :] * g_ref[x - near[0], f] + D * full)
                    g_ref[x - near[0], f] = e
        for e_ref, g_ref, sl, cross, o_sl in sides:
            value = lap(e_ref, 2, 8, 8, planes=8)
            for f in range(2):
                full = value[f] + cross(J1[2:10, f, o_sl, :])
                e = e_ref[2:10, f, 8:16, :] + H * (S[mid, f, sl, :] * g_ref[:, f] + D * full)
                g_ref[:, f] = e

        for copy in y1 + x1:
            copy.wait()
        for e_ref, x, k in ((eW, XO - 2, 2), (eE, XO + 8, 2)):
            t1[x : x + 2, :, OWN, :] = t1[x : x + 2, :, OWN, :] + e_ref[k : k + 2, :, OWN, :]
        for e_ref, g_ref, sl, cross, o_sl in sides:
            t1[mid, :, sl, :] = t1[mid, :, sl, :] + e_ref[2:10, :, 8:16, :]

        def put2(p, sl, cross):
            xv = cross(t1)
            J2[p + 2, :, sl, :] = J2[p + 2, :, sl, :] + H * D * xv
            U[p, :, off(sl), :] = U[p, :, off(sl), :] + H * xv
            if last:
                A7[p, :, off(sl), :] = A7[p, :, off(sl), :] + D * xv

        fix_faces(t1, put2)
        fix_inner(t1, put2)

        raised = level == 1

        def own3(p, c):
            for f, value in enumerate(lap_z(J2, p + 2, Z[p])):
                u, v8, v7 = U[p, f], J2[p + 2, f, OWN, :], J1[p + 2, f, OWN, :]
                a8 = S[p + XO, f, OWN, :] * u + D * value
                if last:
                    u8 = acc[p, f] + H * (I0[p + 2, f, OWN, :] + v7)
                    lanes = slice(128 * f, 128 * f + 128)
                    out_u[0, p, :, lanes] = jnp.where(raised, u8 + 4 * H * (v8 - v7), u8)
                    out_v[0, p, :, lanes] = jnp.where(raised, v8 + 4 * H * (a8 - A7[p, f]), v8)
                else:
                    acc[p, f] = acc[p, f] + H * (I0[p + 2, f, OWN, :] + v7 + v8)
                    I0[p + 2, f, OWN, :] = v8 + H * a8
                    U[p, f] = u + H * value
            return c

        faces_first(own3, J2)
        inner(own3, J2)

        for copy in diag1:
            copy.wait()
        for i, (sx, sy) in enumerate(DIAG):
            near, far, sl = corner_in(sx, sy)
            ends2 = unpack2(cr[r, i, 7])
            for q in range(2):
                for f in range(2):
                    t1[near[q], f, sl, :] = t1[near[q], f, sl, :] + ends2[q][f]
        for g_ref, near in ((gW, (-2, -1)), (gE, (8, 9))):
            for x in near:
                for sl, cross, g_sl in ends:
                    q = x - near[0]
                    g_ref[q, :, off(sl), :] = g_ref[q, :, off(sl), :] + H * D * cross(t1[x + XO, :, g_sl, :])
        for e_ref, g_ref, sl, cross, o_sl in sides:
            for x in (0, 1, 6, 7):
                g_ref[x] = g_ref[x] + H * D * cross_x(None, t1, x, sl)

        for copy in y2 + x2:
            copy.wait()
        for g_ref, x in ((gW, XO - 2), (gE, XO + 8)):
            t2[x : x + 2, :, OWN, :] = t2[x : x + 2, :, OWN, :] + g_ref[...]
        for e_ref, g_ref, sl, cross, o_sl in sides:
            t2[mid, :, sl, :] = t2[mid, :, sl, :] + g_ref[...]

        def put3(p, sl, cross):
            xv = cross(t2)
            if last:
                for f in range(2):
                    lanes = slice(128 * f, 128 * f + 128)
                    old = out_v[0, p, off(sl), lanes]
                    out_v[0, p, off(sl), lanes] = jnp.where(raised, old + 4 * H * D * xv[f], old)
            else:
                I0[p + 2, :, sl, :] = I0[p + 2, :, sl, :] + H * D * xv
                U[p, :, off(sl), :] = U[p, :, off(sl), :] + H * xv

        fix_faces(t2, put3)
        fix_inner(t2, put3)
        if not last:
            for i in range(4):
                pack(i, False)
            diag = send_corners(r + 1, 3)
            x0 = send_x(r + 1, 0, I0, 2, T0.at[r + 1])
            y0 = send_y(r + 1, 2, I0, 2, T0.at[r + 1])


def body(u, v, s):
    ext, alone, block = (16, 2, 48, 128), (12, 2, 48, 128), (8, 2, 32, 128)
    vm = lambda *shape: pltpu.VMEM(shape, F32)
    scratch = [vm(*alone)] * 6 + [vm(ROUNDS, *ext)] * 3 + [vm(*ext)] * 2 + [vm(*block)] * 3
    scratch += [vm(6, 2, 48, 128)] * 2 + [vm(12, 2, 24, 128)] * 2
    scratch += [vm(2, 2, 32, 128)] * 2 + [vm(8, 2, 8, 128)] * 2
    scratch += [vm(4, 8, 8, 128), vm(ROUNDS, 4, 8, 8, 128), vm(2, 2, 8, 128), vm(2, 2, 8, 128), vm(*block), pltpu.VMEM((256, 256), jnp.bfloat16)]
    scratch += [pltpu.SemaphoreType.DMA((6,)), pltpu.SemaphoreType.DMA((30,)), pltpu.SemaphoreType.DMA((50,))]
    out = jax.ShapeDtypeStruct((1, 8, 32, 256), F32)
    return pl.pallas_call(
        kernel,
        out_shape=(out, out),
        in_specs=[pl.BlockSpec(memory_space=pltpu.HBM)] * 3,
        out_specs=(pl.BlockSpec(memory_space=pltpu.VMEM),) * 2,
        scratch_shapes=scratch,
        compiler_params=pltpu.CompilerParams(collective_id=0, has_side_effects=True, vmem_limit_bytes=48 * 1024 * 1024),
    )(*[pltpu.with_memory_space_constraint(x, pltpu.HBM) for x in (u, v, s)])


def solution(mesh):
    placed = (P("gx", "gy", None),) * 3
    return jax.shard_map(
        body,
        mesh=mesh,
        in_specs=placed,
        out_specs=(P("level", "gx", "gy", None),) * 2,
        check_vma=False,
    )
```

```python
import functools

import jax
import jax.numpy as jnp
from jax import lax
from jax.experimental import pallas as pl
from jax.experimental.pallas import tpu as pltpu
from jax.sharding import PartitionSpec as P


H = 0.12
D = 0.05
W1 = 4.0 / 3.0
W2 = -1.0 / 12.0
ROUNDS = 3
MESH = pl.DeviceIdType.MESH
F32 = jnp.float32
XO, YO = 4, 8
OWN = slice(YO, YO + 32)
LO, HI = slice(0, 8), slice(40, 48)
RING = (-2, -1, 8, 9)
NEAREST = {0: (-1, -2), -1: (0, 1), 7: (8, 9), 8: (7, 6)}
NEXT = {1: -1, -2: 0, 6: 8, 9: 7}
DIAG = ((1, 1), (1, -1), (-1, 1), (-1, -1))


def rows(shape):
    return lax.broadcasted_iota(jnp.int32, shape, len(shape) - 2)


def turn(x, n):
    return pltpu.roll(x, n % 8, x.ndim - 2)


def from_below(c):
    r = rows(c.shape)
    return jnp.where(r == 0, W1 * turn(c, 1), 0.0) + jnp.where(r < 2, W2 * turn(c, 2), 0.0)


def from_above(c):
    r = rows(c.shape)
    return jnp.where(r == 7, W1 * turn(c, 7), 0.0) + jnp.where(r >= 6, W2 * turn(c, 6), 0.0)


def z_sums(a, b):
    lane = lax.broadcasted_iota(jnp.int32, a.shape, a.ndim - 1)
    ax = a.ndim - 1

    def shifted(n, mask):
        ra, rb = pltpu.roll(a, n % 128, ax), pltpu.roll(b, n % 128, ax)
        return jnp.where(mask, rb, ra), jnp.where(mask, ra, rb)

    l1, l2 = shifted(1, lane < 1), shifted(2, lane < 2)
    r1, r2 = shifted(127, lane >= 127), shifted(126, lane >= 126)
    return [(l1[i] + r1[i], l2[i] + r2[i]) for i in range(2)]


def lap(ref, p, lo, n, planes=None):
    at = (lambda q: q) if planes is None else (lambda q: pl.ds(q, planes))
    mid = [ref[at(p), f, lo : lo + n, :] for f in range(2)]
    zs = z_sums(*mid)
    out = []
    for f in range(2):
        near = zs[f][0] + ref[at(p - 1), f, lo : lo + n, :] + ref[at(p + 1), f, lo : lo + n, :]
        near = near + ref[at(p), f, lo - 1 : lo - 1 + n, :] + ref[at(p), f, lo + 1 : lo + 1 + n, :]
        far = zs[f][1] + ref[at(p - 2), f, lo : lo + n, :] + ref[at(p + 2), f, lo : lo + n, :]
        far = far + ref[at(p), f, lo - 2 : lo - 2 + n, :] + ref[at(p), f, lo + 2 : lo + 2 + n, :]
        out.append(W1 * near + (W2 * far - 7.5 * mid[f]))
    return out


def lap_z(ref, p, zs):
    out = []
    for f in range(2):
        mid = ref[p, f, OWN, :]
        near = ref[p - 1, f, OWN, :] + ref[p + 1, f, OWN, :]
        near = near + (ref[p, f, YO - 1 : YO + 31, :] + ref[p, f, YO + 1 : YO + 33, :])
        far = ref[p - 2, f, OWN, :] + ref[p + 2, f, OWN, :]
        far = far + (ref[p, f, YO - 2 : YO + 30, :] + ref[p, f, YO + 2 : YO + 34, :])
        out.append(W1 * near + (W2 * far - 5.0 * mid) + (1.0 / 12.0) * zs[f])
    return out


def kernel(u_hbm, v_hbm, s_hbm, out_u, out_v, IU, I0, I1, I2, J1, J2, T0, T1, T2, TU, S, U, acc, A7, eW, eE, eS, eN, gW, gE,
           gS, gN, cs, cr, fs, fr, Z, band, lsem, ssem, rsem):
    level = lax.axis_index("level")
    gx, gy = lax.axis_index("gx"), lax.axis_index("gy")
    nx, ny = lax.axis_size("gx"), lax.axis_size("gy")

    def peer(dx, dy):
        return (level, lax.rem(gx + dx + nx, nx), lax.rem(gy + dy + ny, ny))

    around = ((1, 0), (-1, 0), (0, 1), (0, -1)) + DIAG
    barrier = pltpu.get_barrier_semaphore()
    for d in around:
        pl.semaphore_signal(barrier, 1, device_id=peer(*d), device_id_type=MESH)

    loads = []
    for src, dst, off in ((v_hbm, I0, 2), (u_hbm, IU, 2), (s_hbm, S, XO)):
        for f in range(2):
            copy = pltpu.make_async_copy(
                src.at[:, :, 128 * f : 128 * f + 128], dst.at[off : off + 8, f, OWN, :], lsem.at[len(loads)]
            )
            copy.start()
            loads.append(copy)

    zero = jnp.zeros((2, 2, 48, 128), F32)
    for ref in (IU, I0, I1, I2, J1, J2):
        ref[0:2] = zero
        ref[10:12] = zero
        for sl in (LO, HI):
            ref[2:10, :, sl, :] = jnp.zeros((8, 2, 8, 128), F32)
    for ref in (eW, eE):
        ref[...] = jnp.zeros((6, 2, 48, 128), F32)
    for ref in (eS, eN):
        ref[...] = jnp.zeros((12, 2, 24, 128), F32)

    gap = lax.broadcasted_iota(jnp.int32, (256, 256), 0) - lax.broadcasted_iota(jnp.int32, (256, 256), 1)
    gap = jnp.abs(gap)
    gap = jnp.minimum(gap, 256 - gap)
    weight = jnp.where(gap == 0, -30.0, jnp.where(gap == 1, 16.0, jnp.where(gap == 2, -1.0, 0.0)))
    band[...] = weight.astype(jnp.bfloat16)

    for copy in loads:
        copy.wait()

    def along_z(ref, planes):
        rest = jnp.concatenate(
            [jnp.concatenate([ref[p + 2, f, OWN, :] for f in range(2)], axis=1) for p in planes], axis=0
        )
        parts = []
        for _ in range(3):
            parts.append(rest.astype(jnp.bfloat16))
            rest = rest - parts[-1].astype(F32)
        n = 32 * len(planes)
        out = jnp.dot(jnp.concatenate(parts, axis=0), band[...], preferred_element_type=F32)
        out = out[0:n] + (out[n : 2 * n] + out[2 * n : 3 * n])
        for i, p in enumerate(planes):
            for f in range(2):
                Z[p, f] = out[32 * i : 32 * i + 32, 128 * f : 128 * f + 128]

    def send(r, slot, src, dst, dx, dy):
        got = slot + 20 * (r % 2) if slot < 20 else slot + 20
        copy = pltpu.make_async_remote_copy(
            src_ref=src, dst_ref=dst, send_sem=ssem.at[slot], recv_sem=rsem.at[got],
            device_id=peer(dx, dy), device_id_type=MESH,
        )
        copy.start()
        return copy

    def send_x(r, slot, src, off, dst):
        return [
            send(r, slot, src.at[off + 6 : off + 8, :, OWN, :], dst.at[XO - 2 : XO, :, OWN, :], 1, 0),
            send(r, slot + 1, src.at[off : off + 2, :, OWN, :], dst.at[XO + 8 : XO + 10, :, OWN, :], -1, 0),
        ]

    def send_y(r, slot, src, off, dst):
        return [
            send(r, slot, src.at[off : off + 8, :, 32:40, :], dst.at[XO : XO + 8, :, LO, :], 0, 1),
            send(r, slot + 1, src.at[off : off + 8, :, 8:16, :], dst.at[XO : XO + 8, :, HI, :], 0, -1),
        ]

    def pack4(a, b, sy):
        r = rows(a.shape)
        return jnp.where(r >= 4 if sy > 0 else r < 4, b, turn(a, 4))

    def pack2(items, sy):
        r = rows(items[0].shape)
        out = items[0]
        for i in range(1, 4):
            first = ((6 if sy > 0 else 0) + 2 * i) % 8
            out = jnp.where((r == first) | (r == first + 1), turn(items[i], 2 * i), out)
        return out

    def corner(sx, sy):
        near = (6, 7) if sx > 0 else (0, 1)
        far = (4, 5) if sx > 0 else (2, 3)
        return near, far, (slice(32, 40) if sy > 0 else slice(8, 16))

    def corner_in(sx, sy):
        near = (XO - 2, XO - 1) if sx > 0 else (XO + 8, XO + 9)
        far = (XO - 4, XO - 3) if sx > 0 else (XO + 10, XO + 11)
        return near, far, (LO if sy > 0 else HI)

    def start(p, c):
        for f, value in enumerate(lap_z(IU, p + 2, Z[p])):
            U[p, f] = value
            acc[p, f] = IU[p + 2, f, OWN, :]
        return c

    def alone1(p, c):
        for f, value in enumerate(lap_z(I0, p + 2, Z[p])):
            u = U[p, f]
            new = I0[p + 2, f, OWN, :] + H * (S[p + XO, f, OWN, :] * u + D * value)
            I1[p + 2, f, OWN, :] = new
            J1[p + 2, f, OWN, :] = new
            U[p, f] = u + H * value
        return c

    def alone2(p, c):
        for f, value in enumerate(lap_z(I1, p + 2, Z[p])):
            I2[p + 2, f, OWN, :] = I1[p + 2, f, OWN, :] + H * (S[p + XO, f, OWN, :] * U[p, f] + D * value)
        return c

    def cross_x(own, ring, x, sl):
        at = (lambda q: own[q + 2, :, OWN, :]) if sl is OWN and x in RING else (lambda q: ring[q + XO, :, sl, :])
        if x in NEAREST:
            a, b = NEAREST[x]
            return W1 * at(a) + W2 * at(b)
        return W2 * at(NEXT[x])

    ends = ((slice(8, 16), from_below, LO), (slice(32, 40), from_above, HI))

    def fix_ends(ring, p, put):
        for sl, cross, g in ends:
            put(p, sl, lambda ref: cross(ref[p + XO, :, g, :]))

    def fix_faces(ring, put):
        for x in (0, 1, 6, 7):
            put(x, OWN, lambda ref: cross_x(None, ref, x, OWN))
            fix_ends(ring, x, put)

    def fix_inner(ring, put):
        def step(p, c):
            fix_ends(ring, p, put)
            return c

        lax.fori_loop(2, 6, step, 0, unroll=4)

    def off(sl):
        return slice(sl.start - YO, sl.stop - YO)

    def halves(ref, planes, shift, sl):
        return [ref[q + shift, f, sl, :] for f in range(2) for q in planes]

    def pack(i, first):
        sx, sy = DIAG[i]
        near, far, sl = corner(sx, sy)
        for k, ref in ((0, I0), (3, IU))[: 2 if first else 1]:
            for f in range(2):
                cs[i, k + f] = pack4(*[ref[q + 2, f, sl, :] for q in near], sy)
            cs[i, k + 2] = pack2(halves(ref, far, 2, sl), sy)
        if first:
            cs[i, 6] = pack2(halves(S, near, XO, sl), sy)

    def send_corners(r, n):
        return [send(r, 12 + i, cs.at[i, 0:n], cr.at[r, i, 0:n], *DIAG[i]) for i in range(4)]

    def pack1(i):
        near, _, sl = corner(*DIAG[i])
        cs[i, 7] = pack2(halves(I1, near, 2, sl), DIAG[i][1])

    def send_corners1(r):
        copies = []
        for i in range(4):
            pack1(i)
            copies.append(send(r, 16 + i, cs.at[i, 7:8], cr.at[r, i, 7:8], *DIAG[i]))
        return copies

    def unpack2(tile):
        return [[turn(tile, -2 * (q + 2 * f)) for f in range(2)] for q in range(2)]

    def faces_first(step, ref):
        along_z(ref, (0, 1, 6, 7))
        lax.fori_loop(0, 4, lambda i, c: step(i + 4 * (i // 2), c), 0, unroll=4)

    def inner(step, ref):
        along_z(ref, (2, 3, 4, 5))
        lax.fori_loop(2, 6, step, 0, unroll=4)

    x0 = y0 = None
    for r in range(ROUNDS):
        first, last = r == 0, r == ROUNDS - 1
        t0, t1, t2 = T0.at[r], T1.at[r], T2.at[r]
        extra = []
        if first:
            for k, planes in enumerate(((4, 5), (2, 3))):
                for f in range(2):
                    a, b, c, d = [S[q + XO, f, sl, :] for q in planes for sl in (slice(8, 16), slice(32, 40))]
                    i = rows(a.shape)
                    fs[k, f] = jnp.where(i < 2, a, jnp.where(i >= 6, b, jnp.where(i < 4, turn(c, 2), turn(d, 6))))
            faces_first(start, IU)
            inner(start, IU)
            faces_first(alone1, I0)
            for i in range(4):
                pack(i, True)
                pack1(i)
            inner(alone1, I0)
            pl.semaphore_wait(barrier, len(around))
            x0 = send_x(r, 0, I0, 2, t0)
            y0 = send_y(r, 2, I0, 2, t0)
            extra = send_x(r, 20, IU, 2, TU) + send_y(r, 22, IU, 2, TU)
            diag = send_corners(r, 8)
            extra += send_x(r, 24, S, XO, S) + send_y(r, 26, S, XO, S)
            extra += [send(r, 28, fs.at[0], fr.at[0], 1, 0), send(r, 29, fs.at[1], fr.at[1], -1, 0)]
        if first:
            x1, diag1 = send_x(r, 4, I1, 2, t1), []
        else:
            faces_first(alone1, I0)
            diag1 = send_corners1(r)
            x1 = send_x(r, 4, I1, 2, t1)
            inner(alone1, I0)
        y1 = send_y(r, 6, I1, 2, t1)
        faces_first(alone2, I1)
        x2 = send_x(r, 8, I2, 2, t2)
        inner(alone2, I1)
        y2 = send_y(r, 10, I2, 2, t2)

        for copy in y0 + x0 + extra:
            copy.wait()

        def put1(p, sl, cross):
            xv = cross(t0)
            add, grow = H * D * xv, H * xv
            if first:
                xu = cross(TU)
                add, grow = add + H * (S[p + XO, :, sl, :] * xu), grow + xu
            J1[p + 2, :, sl, :] = J1[p + 2, :, sl, :] + add
            U[p, :, off(sl), :] = U[p, :, off(sl), :] + grow

        fix_faces(t0, put1)
        fix_inner(t0, put1)

        def own2(p, c):
            for f, value in enumerate(lap_z(J1, p + 2, Z[p])):
                u = U[p, f]
                a = S[p + XO, f, OWN, :] * u + D * value
                J2[p + 2, f, OWN, :] = J1[p + 2, f, OWN, :] + H * a
                if last:
                    A7[p, f] = a
                U[p, f] = u + H * value
            return c

        faces_first(own2, J1)
        inner(own2, J1)

        for copy in diag:
            copy.wait()
        for i, (sx, sy) in enumerate(DIAG):
            near, far, sl = corner_in(sx, sy)
            for k, ref in ((0, t0), (3, TU))[: 2 if first else 1]:
                ends2 = unpack2(cr[r, i, k + 2])
                for f in range(2):
                    ref[near[1], f, sl, :] = cr[r, i, k + f]
                    ref[near[0], f, sl, :] = turn(cr[r, i, k + f], 4)
                    ref[far[0], f, sl, :] = ends2[0][f]
                    ref[far[1], f, sl, :] = ends2[1][f]
            if first:
                ends2 = unpack2(cr[r, i, 6])
                for q in range(2):
                    for f in range(2):
                        S[near[q], f, sl, :] = ends2[q][f]
        if first:
            for k, x in enumerate((XO - 4, XO + 10)):
                for f in range(2):
                    S[x, f, 8:16, :] = fr[k, f]
                    S[x, f, 32:40, :] = fr[k, f]
                    S[x + 1, f, 8:16, :] = turn(fr[k, f], 6)
                    S[x + 1, f, 32:40, :] = turn(fr[k, f], 2)

        def both(cross, *where):
            xv = cross(I0, t0)
            e, g = H * D * xv, H * xv
            if first:
                xu = cross(IU, TU)
                e, g = e + H * (S[where] * xu), g + xu
            return e, g

        every = slice(None)
        for e_ref, g_ref, near, far, base in ((eW, gW, (-2, -1), (-4, -3), -4), (eE, gE, (8, 9), (10, 11), 6)):
            for x in near:
                e, g = both(lambda own, ring: cross_x(own, ring, x, OWN), x + XO, every, OWN)
                e_ref[x - base, :, OWN, :] = e
                g_ref[x - near[0]] = g
            for x in near + far:
                for sl, cross, g_sl in ends:
                    e, g = both(lambda own, ring: cross(ring[x + XO, :, g_sl, :]), x + XO, every, sl)
                    if x in near:
                        e_ref[x - base, :, sl, :] = e_ref[x - base, :, sl, :] + e
                        g_ref[x - near[0], :, off(sl), :] = g_ref[x - near[0], :, off(sl), :] + g
                    else:
                        e_ref[x - base, :, sl, :] = e
        sides = ((eS, gS, LO, from_above, slice(8, 16)), (eN, gN, HI, from_below, slice(32, 40)))
        mid = slice(XO, XO + 8)
        for e_ref, g_ref, sl, cross, o_sl in sides:
            e, g = both(lambda own, ring: cross(own[2:10, :, o_sl, :]), mid, every, sl)
            e_ref[2:10, :, 8:16, :] = e
            g_ref[...] = g
            for x in (0, 1, 6, 7):
                e, g = both(lambda own, ring: cross_x(own, ring, x, sl), x + XO, every, sl)
                e_ref[x + 2, :, 8:16, :] = e_ref[x + 2, :, 8:16, :] + e
                g_ref[x] = g_ref[x] + g
            for x in RING:
                e, g = both(
                    lambda own, ring: cross_x(own, ring, x, sl) + cross(ring[x + XO, :, o_sl, :]), x + XO, every, sl
                )
                t1[x + XO, :, sl, :] = e

        for e_ref, g_ref, near, base in ((eW, gW, (-2, -1), -4), (eE, gE, (8, 9), 6)):
            for x in near:
                value = lap(e_ref, x - base, YO, 32)
                cx = cross_x(J1, t1, x, OWN)
                for f in range(2):
                    full = value[f] + cx[f]
                    e = e_ref[x - base, f, OWN, :] + H * (S[x + XO, f, OWN, :] * g_ref[x - near[0], f] + D * full)
                    g_ref[x - near[0], f] = e
        for e_ref, g_ref, sl, cross, o_sl in sides:
            value = lap(e_ref, 2, 8, 8, planes=8)
            for f in range(2):
                full = value[f] + cross(J1[2:10, f, o_sl, :])
                e = e_ref[2:10, f, 8:16, :] + H * (S[mid, f, sl, :] * g_ref[:, f] + D * full)
                g_ref[:, f] = e

        for copy in y1 + x1:
            copy.wait()
        for e_ref, x, k in ((eW, XO - 2, 2), (eE, XO + 8, 2)):
            t1[x : x + 2, :, OWN, :] = t1[x : x + 2, :, OWN, :] + e_ref[k : k + 2, :, OWN, :]
        for e_ref, g_ref, sl, cross, o_sl in sides:
            t1[mid, :, sl, :] = t1[mid, :, sl, :] + e_ref[2:10, :, 8:16, :]

        def put2(p, sl, cross):
            xv = cross(t1)
            J2[p + 2, :, sl, :] = J2[p + 2, :, sl, :] + H * D * xv
            U[p, :, off(sl), :] = U[p, :, off(sl), :] + H * xv
            if last:
                A7[p, :, off(sl), :] = A7[p, :, off(sl), :] + D * xv

        fix_faces(t1, put2)
        fix_inner(t1, put2)

        raised = level == 1

        def own3(p, c):
            for f, value in enumerate(lap_z(J2, p + 2, Z[p])):
                u, v8, v7 = U[p, f], J2[p + 2, f, OWN, :], J1[p + 2, f, OWN, :]
                a8 = S[p + XO, f, OWN, :] * u + D * value
                if last:
                    u8 = acc[p, f] + H * (I0[p + 2, f, OWN, :] + v7)
                    lanes = slice(128 * f, 128 * f + 128)
                    out_u[0, p, :, lanes] = jnp.where(raised, u8 + 4 * H * (v8 - v7), u8)
                    out_v[0, p, :, lanes] = jnp.where(raised, v8 + 4 * H * (a8 - A7[p, f]), v8)
                else:
                    acc[p, f] = acc[p, f] + H * (I0[p + 2, f, OWN, :] + v7 + v8)
                    I0[p + 2, f, OWN, :] = v8 + H * a8
                    U[p, f] = u + H * value
            return c

        faces_first(own3, J2)
        inner(own3, J2)

        for copy in diag1:
            copy.wait()
        for i, (sx, sy) in enumerate(DIAG):
            near, far, sl = corner_in(sx, sy)
            ends2 = unpack2(cr[r, i, 7])
            for q in range(2):
                for f in range(2):
                    t1[near[q], f, sl, :] = t1[near[q], f, sl, :] + ends2[q][f]
        for g_ref, near in ((gW, (-2, -1)), (gE, (8, 9))):
            for x in near:
                for sl, cross, g_sl in ends:
                    q = x - near[0]
                    g_ref[q, :, off(sl), :] = g_ref[q, :, off(sl), :] + H * D * cross(t1[x + XO, :, g_sl, :])
        for e_ref, g_ref, sl, cross, o_sl in sides:
            for x in (0, 1, 6, 7):
                g_ref[x] = g_ref[x] + H * D * cross_x(None, t1, x, sl)

        for copy in y2 + x2:
            copy.wait()
        for g_ref, x in ((gW, XO - 2), (gE, XO + 8)):
            t2[x : x + 2, :, OWN, :] = t2[x : x + 2, :, OWN, :] + g_ref[...]
        for e_ref, g_ref, sl, cross, o_sl in sides:
            t2[mid, :, sl, :] = t2[mid, :, sl, :] + g_ref[...]

        def put3(p, sl, cross):
            xv = cross(t2)
            if last:
                for f in range(2):
                    lanes = slice(128 * f, 128 * f + 128)
                    old = out_v[0, p, off(sl), lanes]
                    out_v[0, p, off(sl), lanes] = jnp.where(raised, old + 4 * H * D * xv[f], old)
            else:
                I0[p + 2, :, sl, :] = I0[p + 2, :, sl, :] + H * D * xv
                U[p, :, off(sl), :] = U[p, :, off(sl), :] + H * xv

        fix_faces(t2, put3)
        fix_inner(t2, put3)
        if not last:
            for i in range(4):
                pack(i, False)
            diag = send_corners(r + 1, 3)
            x0 = send_x(r + 1, 0, I0, 2, T0.at[r + 1])
            y0 = send_y(r + 1, 2, I0, 2, T0.at[r + 1])


def body(u, v, s):
    ext, alone, block = (16, 2, 48, 128), (12, 2, 48, 128), (8, 2, 32, 128)
    vm = lambda *shape: pltpu.VMEM(shape, F32)
    scratch = [vm(*alone)] * 6 + [vm(ROUNDS, *ext)] * 3 + [vm(*ext)] * 2 + [vm(*block)] * 3
    scratch += [vm(6, 2, 48, 128)] * 2 + [vm(12, 2, 24, 128)] * 2
    scratch += [vm(2, 2, 32, 128)] * 2 + [vm(8, 2, 8, 128)] * 2
    scratch += [vm(4, 8, 8, 128), vm(ROUNDS, 4, 8, 8, 128), vm(2, 2, 8, 128), vm(2, 2, 8, 128), vm(*block), pltpu.VMEM((256, 256), jnp.bfloat16)]
    scratch += [pltpu.SemaphoreType.DMA((6,)), pltpu.SemaphoreType.DMA((30,)), pltpu.SemaphoreType.DMA((50,))]
    out = jax.ShapeDtypeStruct((1, 8, 32, 256), F32)
    return pl.pallas_call(
        kernel,
        out_shape=(out, out),
        in_specs=[pl.BlockSpec(memory_space=pltpu.HBM)] * 3,
        out_specs=(pl.BlockSpec(memory_space=pltpu.VMEM),) * 2,
        scratch_shapes=scratch,
        compiler_params=pltpu.CompilerParams(collective_id=0, has_side_effects=True, vmem_limit_bytes=48 * 1024 * 1024),
    )(*[pltpu.with_memory_space_constraint(x, pltpu.HBM) for x in (u, v, s)])


def solution(mesh):
    placed = (P("gx", "gy", None),) * 3
    return jax.shard_map(
        body,
        mesh=mesh,
        in_specs=placed,
        out_specs=(P("level", "gx", "gy", None),) * 2,
        check_vma=False,
    )
```
